8 devices in a mesh: batch: 2 (over z, y), col: 4 (over x, core).
Axes of the slice: x: 2, y: 2, z: 1, core: 2. Of those that a mesh axis runs over, the one named last changes fastest.
Arguments:
- lower: bfloat16 [4096, 2048], P('batch', 'col'), parts along dimension 0
- rhs: bfloat16 [4096, 32768], P('batch', 'col'), parts along dimension 0
Outputs:
- output: bfloat16 [4096, 32768], P('batch', 'col'), parts along dimension 0
There are 2 independent parts. The reference program is written for one: setup_inputs(seed, part) draws one part's arguments, and reference() takes and returns one part's arrays. A program takes and returns all parts, laid end to end along the dimension named above; each array names one.
All inputs are finite; a program needn't handle non-finite values.
Results may differ from the reference program's by a relative error of at most 0.001.
Values are sent between devices in bfloat16 or wider.
A program may use at most 1 GiB of HBM per device.

```python
import jax
import jax.numpy as jnp
from jax import lax

N = 2048
BLOCK_SIZE = 256
GROUP = 4
COLS_DEV = 8192

PER_DEV = N // (BLOCK_SIZE * GROUP)
COLUMNS = COLS_DEV * GROUP


def setup_inputs(seed: int = 0, part: int = 0) -> dict:
    base_key = jax.random.fold_in(jax.random.key(seed), part)
    key_lower, key_rhs = jax.random.split(base_key)
    entries = jax.random.normal(key_lower, (N, N), jnp.float32)
    natural = jnp.tril(entries) * (N ** -0.5)
    stored = natural.reshape(N, PER_DEV, GROUP, BLOCK_SIZE).transpose(0, 2, 1, 3).reshape(N, N)
    rhs = jax.random.normal(key_rhs, (N, COLUMNS), jnp.float32)
    return {"lower": stored.astype(jnp.bfloat16), "rhs": rhs.astype(jnp.bfloat16)}


def reference(lower, rhs):
    natural = lower.reshape(N, GROUP, PER_DEV, BLOCK_SIZE).transpose(0, 2, 1, 3).reshape(N, N)
    col_groups = rhs.reshape(N, GROUP, COLS_DEV).transpose(1, 0, 2)

    def one_group(rhs_cols):
        return jnp.dot(natural, rhs_cols, preferred_element_type=jnp.float32).astype(jnp.bfloat16)

    results = lax.map(one_group, col_groups)
    return results.transpose(1, 0, 2).reshape(N, COLUMNS)
```

```python
import jax
import jax.numpy as jnp
from jax import lax
from jax.experimental import pallas as pl
from jax.experimental.pallas import tpu as pltpu
from jax.sharding import PartitionSpec as P

BLOCK = 256
MESH = pl.DeviceIdType.MESH
MIB = 1024 * 1024
EARLY = 5632
TILE = 512


def when(cond, fn):
    if cond is True:
        fn()
    elif cond is not False:
        pl.when(cond)(fn)


def solution(mesh):
    group = mesh.shape["col"]

    def local_product(l_cols, b_cols):
        order, local_width = l_cols.shape
        width = b_cols.shape[1]
        per_dev = local_width // BLOCK
        n_rows = order // BLOCK
        late = width - EARLY
        n_late = late // TILE
        dtype = b_cols.dtype

        def held(row, owner, t):
            low, high = group * t, group * t + group - 1
            if row >= high:
                return True
            if row < low:
                return False
            return owner + low <= row

        def gather_kernel(l_ref, b_ref, *refs):
            x_refs, l_refs = refs[:n_rows], refs[n_rows:2 * n_rows]
            b_vmem, b_sem, own_sem, x_send, x_recv, p_send, p_recv, f_send, f_recv = refs[2 * n_rows:]
            me = lax.axis_index("col")
            across = lax.rem(me + 2, group)
            partner = me + 1 - 2 * lax.rem(me, 2)
            diagonal = lax.rem(partner + 2, group)

            barrier = pltpu.get_barrier_semaphore()
            for peer in (partner, across):
                pl.semaphore_signal(barrier, inc=1, device_id={"col": peer}, device_id_type=MESH)
            pl.semaphore_wait(barrier, 2)

            def panel(row, owner, t):
                start = pl.multiple_of((owner + group * t) * BLOCK, BLOCK)
                return l_refs[row].at[:, pl.ds(start, BLOCK)]

            def mine(row, t):
                return l_ref.at[pl.ds(row * BLOCK, BLOCK), pl.ds(t * BLOCK, BLOCK)]

            def own_copy(row, t):
                return pltpu.make_async_copy(mine(row, t), panel(row, me, t), own_sem.at[row, t])

            def send(row, t, peer, send_sem, recv_sem):
                return pltpu.make_async_remote_copy(
                    src_ref=mine(row, t), dst_ref=panel(row, me, t), send_sem=send_sem.at[row, t],
                    recv_sem=recv_sem.at[row, t], device_id={"col": peer}, device_id_type=MESH)

            def arrival(row, t, owner, recv_sem):
                dst = panel(row, owner, t)
                return pltpu.make_async_remote_copy(
                    src_ref=dst, dst_ref=dst, send_sem=x_send.at[row, t], recv_sem=recv_sem.at[row, t],
                    device_id={"col": partner}, device_id_type=MESH)

            def forward(row, t):
                block = panel(row, across, t)
                return pltpu.make_async_remote_copy(
                    src_ref=block, dst_ref=block, send_sem=f_send.at[row, t], recv_sem=f_recv.at[row, t],
                    device_id={"col": partner}, device_id_type=MESH)

            def load_b(k):
                rows = pl.ds(k * BLOCK, BLOCK)
                return pltpu.make_async_copy(b_ref.at[rows, pl.ds(0, EARLY)], b_vmem.at[rows, :], b_sem.at[k])

            sequence = list(range(n_rows - 1, -1, -1))
            blocks = [(row, t) for row in sequence for t in range(per_dev)]
            for row, t in blocks:
                when(held(row, me, t), lambda row=row, t=t: send(row, t, across, x_send, x_recv).start())
            for row, t in blocks:
                def start_near(row=row, t=t):
                    send(row, t, partner, p_send, p_recv).start()
                    own_copy(row, t).start()
                when(held(row, me, t), start_near)
            for k in range(n_rows):
                load_b(k).start()

            def relay(row):
                for t in range(per_dev):
                    def step(t=t):
                        arrival(row, t, across, x_recv).wait_recv()
                        forward(row, t).start()
                    when(held(row, across, t), step)

            def multiply(row, first, last, step):
                depth = (row + 1) * BLOCK

                def body(n, carry):
                    cols = pl.ds(pl.multiple_of(n * step, TILE), step)
                    x_refs[row][:, cols] = jnp.dot(
                        l_refs[row][...], b_vmem[pl.ds(0, depth), cols],
                        preferred_element_type=jnp.float32).astype(dtype)
                    return carry

                lax.fori_loop(first, last, body, 0)

            relay(sequence[0])
            for place, row in enumerate(sequence):
                for t in range(per_dev):
                    when(held(row, me, t), lambda t=t: own_copy(row, t).wait())
                    when(held(row, partner, t), lambda t=t: arrival(row, t, partner, p_recv).wait_recv())
                    when(held(row, diagonal, t), lambda t=t: arrival(row, t, diagonal, f_recv).wait_recv())
                if place == 0:
                    for k in range(n_rows):
                        load_b(k).wait()
                step = TILE
                count = EARLY // step
                split = (count * 3) // 4
                multiply(row, 0, split, step)
                if place + 1 < n_rows:
                    relay(sequence[place + 1])
                multiply(row, split, count, step)

            for row, t in blocks:
                def drain(row=row, t=t):
                    send(row, t, across, x_send, x_recv).wait_send()
                    send(row, t, partner, p_send, p_recv).wait_send()
                when(held(row, me, t), drain)
                when(held(row, across, t), lambda row=row, t=t: forward(row, t).wait_send())

        dma = pltpu.SemaphoreType.DMA
        vmem = pl.BlockSpec(memory_space=pltpu.VMEM)
        hbm = pl.BlockSpec(memory_space=pl.ANY)
        gathered = pl.pallas_call(
            gather_kernel,
            out_shape=tuple(pltpu.VMEM((BLOCK, EARLY), dtype) for _ in range(n_rows))
            + tuple(pltpu.VMEM((BLOCK, BLOCK * (i + 1)), dtype) for i in range(n_rows)),
            in_specs=[hbm, hbm],
            out_specs=(vmem,) * (2 * n_rows),
            scratch_shapes=[pltpu.VMEM((order, EARLY), dtype), dma((n_rows,))] + [dma((n_rows, per_dev))] * 7,
            compiler_params=pltpu.CompilerParams(
                collective_id=0, has_side_effects=True, vmem_limit_bytes=27 * MIB),
            name="gather_and_multiply",
        )(l_cols, b_cols)

        def finish_kernel(*refs):
            x_refs, l_refs = refs[:n_rows], refs[n_rows:2 * n_rows]
            b_ref, out_ref, b_vmem, x_vmem, b_sem, x_sem, early_sem = refs[2 * n_rows:]

            def load_b(n):
                return pltpu.make_async_copy(
                    b_ref.at[:, pl.ds(pl.multiple_of(EARLY + n * TILE, TILE), TILE)], b_vmem.at[n], b_sem.at[n])

            def put_early(row):
                return pltpu.make_async_copy(
                    x_refs[row], out_ref.at[pl.ds(row * BLOCK, BLOCK), pl.ds(0, EARLY)], early_sem.at[row])

            def put_late(n):
                return pltpu.make_async_copy(
                    x_vmem.at[n], out_ref.at[:, pl.ds(pl.multiple_of(EARLY + n * TILE, TILE), TILE)], x_sem.at[n])

            for n in range(n_late):
                load_b(n).start()
            for row in range(n_rows):
                put_early(row).start()

            def body(n, carry):
                load_b(n).wait()
                for row in range(n_rows - 1, -1, -1):
                    depth = (row + 1) * BLOCK
                    x_vmem[n, pl.ds(row * BLOCK, BLOCK), :] = jnp.dot(
                        l_refs[row][...], b_vmem[n, pl.ds(0, depth), :],
                        preferred_element_type=jnp.float32).astype(dtype)
                put_late(n).start()
                return carry

            lax.fori_loop(0, n_late, body, 0)
            for n in range(n_late):
                put_late(n).wait()
            for row in range(n_rows):
                put_early(row).wait()

        return pl.pallas_call(
            finish_kernel,
            out_shape=jax.ShapeDtypeStruct((order, width), dtype),
            in_specs=[vmem] * (2 * n_rows) + [hbm],
            out_specs=hbm,
            scratch_shapes=[
                pltpu.VMEM((n_late, order, TILE), dtype), pltpu.VMEM((n_late, order, TILE), dtype),
                dma((n_late,)), dma((n_late,)), dma((n_rows,))],
            compiler_params=pltpu.CompilerParams(vmem_limit_bytes=26 * MIB),
            name="finish",
        )(*gathered, b_cols)

    return jax.shard_map(local_product, mesh=mesh, in_specs=(P("batch", "col"), P("batch", "col")), out_specs=P("batch", "col"), check_vma=False)
```

```python
import jax
import jax.numpy as jnp
from jax import lax
from jax.experimental import pallas as pl
from jax.experimental.pallas import tpu as pltpu
from jax.sharding import PartitionSpec as P

BLOCK = 256
MESH = pl.DeviceIdType.MESH
MIB = 1024 * 1024
EARLY = 5632
TILE = 512


def when(cond, fn):
    if cond is True:
        fn()
    elif cond is not False:
        pl.when(cond)(fn)


def solution(mesh):
    group = mesh.shape["col"]

    def local_product(l_cols, b_cols):
        order, local_width = l_cols.shape
        width = b_cols.shape[1]
        per_dev = local_width // BLOCK
        n_rows = order // BLOCK
        late = width - EARLY
        n_late = late // TILE
        dtype = b_cols.dtype

        def held(row, owner, t):
            low, high = group * t, group * t + group - 1
            if row >= high:
                return True
            if row < low:
                return False
            return owner + low <= row

        def gather_kernel(l_ref, b_ref, *refs):
            x_refs, l_refs = refs[:n_rows], refs[n_rows:2 * n_rows]
            b_vmem, b_sem, own_sem, x_send, x_recv, p_send, p_recv, f_send, f_recv = refs[2 * n_rows:]
            me = lax.axis_index("col")
            across = lax.rem(me + 2, group)
            partner = me + 1 - 2 * lax.rem(me, 2)
            diagonal = lax.rem(partner + 2, group)

            barrier = pltpu.get_barrier_semaphore()
            for peer in (partner, across):
                pl.semaphore_signal(barrier, inc=1, device_id={"col": peer}, device_id_type=MESH)
            pl.semaphore_wait(barrier, 2)

            def panel(row, owner, t):
                start = pl.multiple_of((owner + group * t) * BLOCK, BLOCK)
                return l_refs[row].at[:, pl.ds(start, BLOCK)]

            def mine(row, t):
                return l_ref.at[pl.ds(row * BLOCK, BLOCK), pl.ds(t * BLOCK, BLOCK)]

            def own_copy(row, t):
                return pltpu.make_async_copy(mine(row, t), panel(row, me, t), own_sem.at[row, t])

            def send(row, t, peer, send_sem, recv_sem):
                return pltpu.make_async_remote_copy(
                    src_ref=mine(row, t), dst_ref=panel(row, me, t), send_sem=send_sem.at[row, t],
                    recv_sem=recv_sem.at[row, t], device_id={"col": peer}, device_id_type=MESH)

            def arrival(row, t, owner, recv_sem):
                dst = panel(row, owner, t)
                return pltpu.make_async_remote_copy(
                    src_ref=dst, dst_ref=dst, send_sem=x_send.at[row, t], recv_sem=recv_sem.at[row, t],
                    device_id={"col": partner}, device_id_type=MESH)

            def forward(row, t):
                block = panel(row, across, t)
                return pltpu.make_async_remote_copy(
                    src_ref=block, dst_ref=block, send_sem=f_send.at[row, t], recv_sem=f_recv.at[row, t],
                    device_id={"col": partner}, device_id_type=MESH)

            def load_b(k):
                rows = pl.ds(k * BLOCK, BLOCK)
                return pltpu.make_async_copy(b_ref.at[rows, pl.ds(0, EARLY)], b_vmem.at[rows, :], b_sem.at[k])

            sequence = [3, 7, 6, 5, 4, 2, 1, 0]
            blocks = [(row, t) for row in sequence for t in range(per_dev)]
            for row, t in blocks:
                when(held(row, me, t), lambda row=row, t=t: send(row, t, across, x_send, x_recv).start())
            for row, t in blocks:
                def start_near(row=row, t=t):
                    send(row, t, partner, p_send, p_recv).start()
                    own_copy(row, t).start()
                when(held(row, me, t), start_near)
            for k in range(n_rows):
                load_b(k).start()

            def relay(row):
                for t in range(per_dev):
                    def step(t=t):
                        arrival(row, t, across, x_recv).wait_recv()
                        forward(row, t).start()
                    when(held(row, across, t), step)

            def multiply(row, start, stop):
                depth = (row + 1) * BLOCK
                x_refs[row][:, start:stop] = jnp.dot(
                    l_refs[row][...], b_vmem[:depth, start:stop],
                    preferred_element_type=jnp.float32).astype(dtype)

            relay(sequence[0])
            loaded = 0
            for place, row in enumerate(sequence):
                for t in range(per_dev):
                    when(held(row, me, t), lambda t=t: own_copy(row, t).wait())
                    when(held(row, partner, t), lambda t=t: arrival(row, t, partner, p_recv).wait_recv())
                    when(held(row, diagonal, t), lambda t=t: arrival(row, t, diagonal, f_recv).wait_recv())
                for k in range(loaded, row + 1):
                    load_b(k).wait()
                loaded = max(loaded, row + 1)
                split = EARLY // (2 * TILE) * TILE
                multiply(row, 0, split)
                if place + 1 < n_rows:
                    relay(sequence[place + 1])
                multiply(row, split, EARLY)

            for row, t in blocks:
                def drain(row=row, t=t):
                    send(row, t, across, x_send, x_recv).wait_send()
                    send(row, t, partner, p_send, p_recv).wait_send()
                when(held(row, me, t), drain)
                when(held(row, across, t), lambda row=row, t=t: forward(row, t).wait_send())

        dma = pltpu.SemaphoreType.DMA
        vmem = pl.BlockSpec(memory_space=pltpu.VMEM)
        hbm = pl.BlockSpec(memory_space=pl.ANY)
        gathered = pl.pallas_call(
            gather_kernel,
            out_shape=tuple(pltpu.VMEM((BLOCK, EARLY), dtype) for _ in range(n_rows))
            + tuple(pltpu.VMEM((BLOCK, BLOCK * (i + 1)), dtype) for i in range(n_rows)),
            in_specs=[hbm, hbm],
            out_specs=(vmem,) * (2 * n_rows),
            scratch_shapes=[pltpu.VMEM((order, EARLY), dtype), dma((n_rows,))] + [dma((n_rows, per_dev))] * 7,
            compiler_params=pltpu.CompilerParams(
                collective_id=0, has_side_effects=True, vmem_limit_bytes=27 * MIB),
            name="gather_and_multiply",
        )(l_cols, b_cols)

        def finish_kernel(*refs):
            x_refs, l_refs = refs[:n_rows], refs[n_rows:2 * n_rows]
            b_ref, out_ref, b_vmem, x_vmem, b_sem, x_sem, early_sem = refs[2 * n_rows:]

            def load_b(n):
                return pltpu.make_async_copy(
                    b_ref.at[:, pl.ds(pl.multiple_of(EARLY + n * TILE, TILE), TILE)], b_vmem.at[n], b_sem.at[n])

            def put_early(row):
                return pltpu.make_async_copy(
                    x_refs[row], out_ref.at[pl.ds(row * BLOCK, BLOCK), pl.ds(0, EARLY)], early_sem.at[row])

            def put_late(n):
                return pltpu.make_async_copy(
                    x_vmem.at[n], out_ref.at[:, pl.ds(pl.multiple_of(EARLY + n * TILE, TILE), TILE)], x_sem.at[n])

            for n in range(n_late):
                load_b(n).start()
            for row in range(n_rows):
                put_early(row).start()

            def body(n, carry):
                load_b(n).wait()
                for row in range(n_rows - 1, -1, -1):
                    depth = (row + 1) * BLOCK
                    x_vmem[n, pl.ds(row * BLOCK, BLOCK), :] = jnp.dot(
                        l_refs[row][...], b_vmem[n, pl.ds(0, depth), :],
                        preferred_element_type=jnp.float32).astype(dtype)
                put_late(n).start()
                return carry

            lax.fori_loop(0, n_late, body, 0)
            for n in range(n_late):
                put_late(n).wait()
            for row in range(n_rows):
                put_early(row).wait()

        return pl.pallas_call(
            finish_kernel,
            out_shape=jax.ShapeDtypeStruct((order, width), dtype),
            in_specs=[vmem] * (2 * n_rows) + [hbm],
            out_specs=hbm,
            scratch_shapes=[
                pltpu.VMEM((n_late, order, TILE), dtype), pltpu.VMEM((n_late, order, TILE), dtype),
                dma((n_late,)), dma((n_late,)), dma((n_rows,))],
            compiler_params=pltpu.CompilerParams(vmem_limit_bytes=26 * MIB),
            name="finish",
        )(*gathered, b_cols)

    return jax.shard_map(local_product, mesh=mesh, in_specs=(P("batch", "col"), P("batch", "col")), out_specs=P("batch", "col"), check_vma=False)
```

```python
import jax
import jax.numpy as jnp
from jax import lax
from jax.experimental import pallas as pl
from jax.experimental.pallas import tpu as pltpu
from jax.sharding import PartitionSpec as P

BLOCK = 256
MESH = pl.DeviceIdType.MESH
MIB = 1024 * 1024
EARLY = 5632
TILE = 512


def when(cond, fn):
    if cond is True:
        fn()
    elif cond is not False:
        pl.when(cond)(fn)


def solution(mesh):
    group = mesh.shape["col"]

    def local_product(l_cols, b_cols):
        order, local_width = l_cols.shape
        width = b_cols.shape[1]
        per_dev = local_width // BLOCK
        n_rows = order // BLOCK
        late = width - EARLY
        n_late = late // TILE
        dtype = b_cols.dtype

        def held(row, owner, t):
            low, high = group * t, group * t + group - 1
            if row >= high:
                return True
            if row < low:
                return False
            return owner + low <= row

        def gather_kernel(l_ref, b_ref, *refs):
            x_refs, l_refs = refs[:n_rows], refs[n_rows:2 * n_rows]
            b_first, b_vmem, b_sem, own_sem, x_send, x_recv, p_send, p_recv, f_send, f_recv = refs[2 * n_rows:]
            me = lax.axis_index("col")
            across = lax.rem(me + 2, group)
            partner = me + 1 - 2 * lax.rem(me, 2)
            diagonal = lax.rem(partner + 2, group)

            barrier = pltpu.get_barrier_semaphore()
            for peer in (partner, across):
                pl.semaphore_signal(barrier, inc=1, device_id={"col": peer}, device_id_type=MESH)
            pl.semaphore_wait(barrier, 2)

            def panel(row, owner, t):
                start = pl.multiple_of((owner + group * t) * BLOCK, BLOCK)
                return l_refs[row].at[:, pl.ds(start, BLOCK)]

            def mine(row, t):
                return l_ref.at[pl.ds(row * BLOCK, BLOCK), pl.ds(t * BLOCK, BLOCK)]

            def own_copy(row, t):
                return pltpu.make_async_copy(mine(row, t), panel(row, me, t), own_sem.at[row, t])

            def send(row, t, peer, send_sem, recv_sem):
                return pltpu.make_async_remote_copy(
                    src_ref=mine(row, t), dst_ref=panel(row, me, t), send_sem=send_sem.at[row, t],
                    recv_sem=recv_sem.at[row, t], device_id={"col": peer}, device_id_type=MESH)

            def arrival(row, t, owner, recv_sem):
                dst = panel(row, owner, t)
                return pltpu.make_async_remote_copy(
                    src_ref=dst, dst_ref=dst, send_sem=x_send.at[row, t], recv_sem=recv_sem.at[row, t],
                    device_id={"col": partner}, device_id_type=MESH)

            def forward(row, t):
                block = panel(row, across, t)
                return pltpu.make_async_remote_copy(
                    src_ref=block, dst_ref=block, send_sem=f_send.at[row, t], recv_sem=f_recv.at[row, t],
                    device_id={"col": partner}, device_id_type=MESH)

            def load_b(k):
                rows = pl.ds(k * BLOCK, BLOCK)
                return pltpu.make_async_copy(b_ref.at[rows, pl.ds(0, EARLY)], b_vmem.at[rows, :], b_sem.at[k])

            first_late = pltpu.make_async_copy(b_ref.at[:, pl.ds(EARLY, TILE)], b_first, b_sem.at[n_rows])
            sequence = [3, 7, 6, 5, 4, 2, 1, 0]
            blocks = [(row, t) for row in sequence for t in range(per_dev)]
            for row, t in blocks:
                when(held(row, me, t), lambda row=row, t=t: send(row, t, across, x_send, x_recv).start())
            for row, t in blocks:
                def start_near(row=row, t=t):
                    send(row, t, partner, p_send, p_recv).start()
                    own_copy(row, t).start()
                when(held(row, me, t), start_near)
            for k in range(n_rows):
                load_b(k).start()
            first_late.start()

            def relay(row):
                for t in range(per_dev):
                    def step(t=t):
                        arrival(row, t, across, x_recv).wait_recv()
                        forward(row, t).start()
                    when(held(row, across, t), step)

            def multiply(row, start, stop):
                depth = (row + 1) * BLOCK
                x_refs[row][:, start:stop] = jnp.dot(
                    l_refs[row][...], b_vmem[:depth, start:stop],
                    preferred_element_type=jnp.float32).astype(dtype)

            relay(sequence[0])
            loaded = 0
            for place, row in enumerate(sequence):
                for t in range(per_dev):
                    when(held(row, me, t), lambda t=t: own_copy(row, t).wait())
                    when(held(row, partner, t), lambda t=t: arrival(row, t, partner, p_recv).wait_recv())
                    when(held(row, diagonal, t), lambda t=t: arrival(row, t, diagonal, f_recv).wait_recv())
                for k in range(loaded, row + 1):
                    load_b(k).wait()
                loaded = max(loaded, row + 1)
                split = EARLY // (2 * TILE) * TILE
                multiply(row, 0, split)
                if place + 1 < n_rows:
                    relay(sequence[place + 1])
                multiply(row, split, EARLY)

            first_late.wait()
            for row, t in blocks:
                def drain(row=row, t=t):
                    send(row, t, across, x_send, x_recv).wait_send()
                    send(row, t, partner, p_send, p_recv).wait_send()
                when(held(row, me, t), drain)
                when(held(row, across, t), lambda row=row, t=t: forward(row, t).wait_send())

        dma = pltpu.SemaphoreType.DMA
        vmem = pl.BlockSpec(memory_space=pltpu.VMEM)
        hbm = pl.BlockSpec(memory_space=pl.ANY)
        gathered = pl.pallas_call(
            gather_kernel,
            out_shape=tuple(pltpu.VMEM((BLOCK, EARLY), dtype) for _ in range(n_rows))
            + tuple(pltpu.VMEM((BLOCK, BLOCK * (i + 1)), dtype) for i in range(n_rows))
            + (pltpu.VMEM((order, TILE), dtype),),
            in_specs=[hbm, hbm],
            out_specs=(vmem,) * (2 * n_rows + 1),
            scratch_shapes=[pltpu.VMEM((order, EARLY), dtype), dma((n_rows + 1,))] + [dma((n_rows, per_dev))] * 7,
            compiler_params=pltpu.CompilerParams(
                collective_id=0, has_side_effects=True, vmem_limit_bytes=24 * MIB),
            name="gather_and_multiply",
        )(l_cols, b_cols)

        def finish_kernel(*refs):
            x_refs, l_refs = refs[:n_rows], refs[n_rows:2 * n_rows]
            b_first, b_ref, out_ref, b_vmem, x_vmem, b_sem, x_sem, early_sem = refs[2 * n_rows:]

            def load_b(n):
                cols = pl.ds(pl.multiple_of(EARLY + n * TILE, TILE), TILE)
                return pltpu.make_async_copy(b_ref.at[:, cols], b_vmem.at[n - 1], b_sem.at[n - 1])

            def put_early(row):
                return pltpu.make_async_copy(
                    x_refs[row], out_ref.at[pl.ds(row * BLOCK, BLOCK), pl.ds(0, EARLY)], early_sem.at[row])

            def put_late(n, row):
                rows = pl.ds(row * BLOCK, BLOCK)
                cols = pl.ds(pl.multiple_of(EARLY + n * TILE, TILE), TILE)
                return pltpu.make_async_copy(x_vmem.at[n, rows, :], out_ref.at[rows, cols], x_sem.at[n, row])

            def multiply(n, b_tile):
                for row in range(n_rows - 1, -1, -1):
                    x_vmem[n, pl.ds(row * BLOCK, BLOCK), :] = jnp.dot(
                        l_refs[row][...], b_tile[pl.ds(0, (row + 1) * BLOCK), :],
                        preferred_element_type=jnp.float32).astype(dtype)
                    put_late(n, row).start()

            load_b(1).start()
            load_b(2).start()
            for row in range(n_rows - 1, 4, -1):
                put_early(row).start()
            multiply(0, b_first)

            def body(n, carry):
                @pl.when(n + 2 < n_late)
                def _():
                    load_b(n + 2).start()
                for row in range(5):
                    when(n == 1 + row // 2, lambda row=row: put_early(row).start())
                load_b(n).wait()
                multiply(n, b_vmem.at[n - 1])
                return carry

            lax.fori_loop(1, n_late, body, 0)
            for row in range(n_rows):
                put_early(row).wait()

            def drain(n, carry):
                for row in range(n_rows):
                    put_late(n, row).wait()
                return carry

            lax.fori_loop(0, n_late, drain, 0)

        return pl.pallas_call(
            finish_kernel,
            out_shape=jax.ShapeDtypeStruct((order, width), dtype),
            in_specs=[vmem] * (2 * n_rows + 1) + [hbm],
            out_specs=hbm,
            scratch_shapes=[
                pltpu.VMEM((n_late - 1, order, TILE), dtype), pltpu.VMEM((n_late, order, TILE), dtype),
                dma((n_late - 1,)), dma((n_late, n_rows)), dma((n_rows,))],
            compiler_params=pltpu.CompilerParams(vmem_limit_bytes=20 * MIB),
            name="finish",
        )(*gathered, b_cols)

    return jax.shard_map(local_product, mesh=mesh, in_specs=(P("batch", "col"), P("batch", "col")), out_specs=P("batch", "col"), check_vma=False)
```

```python
import jax
import jax.numpy as jnp
from jax import lax
from jax.experimental import pallas as pl
from jax.experimental.pallas import tpu as pltpu
from jax.sharding import PartitionSpec as P

BLOCK = 256
MESH = pl.DeviceIdType.MESH
MIB = 1024 * 1024
EARLY = 5632
TILE = 512


def when(cond, fn):
    if cond is True:
        fn()
    elif cond is not False:
        pl.when(cond)(fn)


def solution(mesh):
    group = mesh.shape["col"]

    def local_product(l_cols, b_cols):
        order, local_width = l_cols.shape
        width = b_cols.shape[1]
        per_dev = local_width // BLOCK
        n_rows = order // BLOCK
        late = width - EARLY
        n_late = late // TILE
        dtype = b_cols.dtype

        def held(row, owner, t):
            low, high = group * t, group * t + group - 1
            if row >= high:
                return True
            if row < low:
                return False
            return owner + low <= row

        def late_place(k):
            return pl.ds((n_rows - 1 - k // 2) * BLOCK, BLOCK), (k % 2) * late

        def gather_kernel(l_ref, b_ref, *refs):
            x_refs, l_refs = refs[:n_rows], refs[n_rows:2 * n_rows]
            b_vmem, b_sem, late_sem, own_sem, x_send, x_recv, p_send, p_recv, f_send, f_recv = refs[2 * n_rows:]
            me = lax.axis_index("col")
            across = lax.rem(me + 2, group)
            partner = me + 1 - 2 * lax.rem(me, 2)
            diagonal = lax.rem(partner + 2, group)

            barrier = pltpu.get_barrier_semaphore()
            for peer in (partner, across):
                pl.semaphore_signal(barrier, inc=1, device_id={"col": peer}, device_id_type=MESH)
            pl.semaphore_wait(barrier, 2)

            def panel(row, owner, t):
                start = pl.multiple_of((owner + group * t) * BLOCK, BLOCK)
                return l_refs[row].at[:, pl.ds(start, BLOCK)]

            def mine(row, t):
                return l_ref.at[pl.ds(row * BLOCK, BLOCK), pl.ds(t * BLOCK, BLOCK)]

            def own_copy(row, t):
                return pltpu.make_async_copy(mine(row, t), panel(row, me, t), own_sem.at[row, t])

            def send(row, t, peer, send_sem, recv_sem):
                return pltpu.make_async_remote_copy(
                    src_ref=mine(row, t), dst_ref=panel(row, me, t), send_sem=send_sem.at[row, t],
                    recv_sem=recv_sem.at[row, t], device_id={"col": peer}, device_id_type=MESH)

            def arrival(row, t, owner, recv_sem):
                dst = panel(row, owner, t)
                return pltpu.make_async_remote_copy(
                    src_ref=dst, dst_ref=dst, send_sem=x_send.at[row, t], recv_sem=recv_sem.at[row, t],
                    device_id={"col": partner}, device_id_type=MESH)

            def forward(row, t):
                block = panel(row, across, t)
                return pltpu.make_async_remote_copy(
                    src_ref=block, dst_ref=block, send_sem=f_send.at[row, t], recv_sem=f_recv.at[row, t],
                    device_id={"col": partner}, device_id_type=MESH)

            def load_b(k):
                rows = pl.ds(k * BLOCK, BLOCK)
                return pltpu.make_async_copy(b_ref.at[rows, pl.ds(0, EARLY)], b_vmem.at[rows, :], b_sem.at[k])

            def load_late(k):
                rows, start = late_place(k)
                return pltpu.make_async_copy(
                    b_ref.at[pl.ds(k * BLOCK, BLOCK), pl.ds(EARLY, late)], b_vmem.at[rows, pl.ds(start, late)], late_sem.at[k])

            sequence = [3, 7, 6, 5, 4, 2, 1, 0]
            blocks = [(row, t) for row in sequence for t in range(per_dev)]
            for row, t in blocks:
                when(held(row, me, t), lambda row=row, t=t: send(row, t, across, x_send, x_recv).start())
            for row, t in blocks:
                def start_near(row=row, t=t):
                    send(row, t, partner, p_send, p_recv).start()
                    own_copy(row, t).start()
                when(held(row, me, t), start_near)
            for k in range(n_rows):
                load_b(k).start()

            def relay(row):
                for t in range(per_dev):
                    def step(t=t):
                        arrival(row, t, across, x_recv).wait_recv()
                        forward(row, t).start()
                    when(held(row, across, t), step)

            def multiply(row, start, stop):
                depth = (row + 1) * BLOCK
                x_refs[row][:, start:stop] = jnp.dot(
                    l_refs[row][...], b_vmem[:depth, start:stop],
                    preferred_element_type=jnp.float32).astype(dtype)

            relay(sequence[0])
            loaded = 0
            for place, row in enumerate(sequence):
                for t in range(per_dev):
                    when(held(row, me, t), lambda t=t: own_copy(row, t).wait())
                    when(held(row, partner, t), lambda t=t: arrival(row, t, partner, p_recv).wait_recv())
                    when(held(row, diagonal, t), lambda t=t: arrival(row, t, diagonal, f_recv).wait_recv())
                for k in range(loaded, row + 1):
                    load_b(k).wait()
                loaded = max(loaded, row + 1)
                split = EARLY // (2 * TILE) * TILE
                multiply(row, 0, split)
                if place + 1 < n_rows:
                    relay(sequence[place + 1])
                multiply(row, split, EARLY)
                if row >= n_rows // 2:
                    for k in range(2 * (n_rows - 1 - row), 2 * (n_rows - row)):
                        load_late(k).start()

            for k in range(n_rows):
                load_late(k).wait()
            for row, t in blocks:
                def drain(row=row, t=t):
                    send(row, t, across, x_send, x_recv).wait_send()
                    send(row, t, partner, p_send, p_recv).wait_send()
                when(held(row, me, t), drain)
                when(held(row, across, t), lambda row=row, t=t: forward(row, t).wait_send())

        dma = pltpu.SemaphoreType.DMA
        vmem = pl.BlockSpec(memory_space=pltpu.VMEM)
        hbm = pl.BlockSpec(memory_space=pltpu.HBM)
        gathered = pl.pallas_call(
            gather_kernel,
            out_shape=tuple(pltpu.VMEM((BLOCK, EARLY), dtype) for _ in range(n_rows))
            + tuple(pltpu.VMEM((BLOCK, BLOCK * (i + 1)), dtype) for i in range(n_rows))
            + (pltpu.VMEM((order, EARLY), dtype),),
            in_specs=[hbm, hbm],
            out_specs=(vmem,) * (2 * n_rows + 1),
            scratch_shapes=[dma((n_rows,)), dma((n_rows,))] + [dma((n_rows, per_dev))] * 7,
            compiler_params=pltpu.CompilerParams(
                collective_id=0, has_side_effects=True, vmem_limit_bytes=5 * MIB),
            name="gather_and_multiply",
        )(l_cols, b_cols)

        def finish_kernel(*refs):
            x_refs, l_refs = refs[:n_rows], refs[n_rows:2 * n_rows]
            b_vmem, out_ref, x_vmem, x_sem, early_sem = refs[2 * n_rows:]

            def put_early(row):
                return pltpu.make_async_copy(
                    x_refs[row], out_ref.at[pl.ds(row * BLOCK, BLOCK), pl.ds(0, EARLY)], early_sem.at[row])

            def put_late(n, row):
                rows = pl.ds(row * BLOCK, BLOCK)
                cols = pl.ds(pl.multiple_of(EARLY + n * TILE, TILE), TILE)
                slot = lax.rem(n, 2)
                return pltpu.make_async_copy(x_vmem.at[slot, rows, :], out_ref.at[rows, cols], x_sem.at[slot, row])

            for row in range(n_rows - 1, 4, -1):
                put_early(row).start()

            def body(n, carry):
                for row in range(5):
                    when(n == 1 + row // 2, lambda row=row: put_early(row).start())

                @pl.when(n >= 2)
                def _():
                    for row in range(n_rows):
                        put_late(n - 2, row).wait()

                for row in range(n_rows - 1, -1, -1):
                    total = None
                    for k in range(row + 1):
                        rows, start = late_place(k)
                        cols = pl.ds(pl.multiple_of(start + n * TILE, TILE), TILE)
                        term = jnp.dot(l_refs[row][:, k * BLOCK:(k + 1) * BLOCK], b_vmem[rows, cols],
                                       preferred_element_type=jnp.float32)
                        total = term if total is None else total + term
                    x_vmem[lax.rem(n, 2), pl.ds(row * BLOCK, BLOCK), :] = total.astype(dtype)
                    put_late(n, row).start()
                return carry

            lax.fori_loop(0, n_late, body, 0)
            for row in range(n_rows):
                put_early(row).wait()
            for n in range(n_late - 2, n_late):
                for row in range(n_rows):
                    put_late(n, row).wait()

        return pl.pallas_call(
            finish_kernel,
            out_shape=jax.ShapeDtypeStruct((order, width), dtype),
            in_specs=[vmem] * (2 * n_rows + 1),
            out_specs=hbm,
            scratch_shapes=[pltpu.VMEM((2, order, TILE), dtype), dma((2, n_rows)), dma((n_rows,))],
            compiler_params=pltpu.CompilerParams(vmem_limit_bytes=5 * MIB),
            name="finish",
        )(*gathered)

    return jax.shard_map(local_product, mesh=mesh, in_specs=(P("batch", "col"), P("batch", "col")), out_specs=P("batch", "col"), check_vma=False)
```

```python
import jax
import jax.numpy as jnp
from jax import lax
from jax.experimental import pallas as pl
from jax.experimental.pallas import tpu as pltpu
from jax.sharding import PartitionSpec as P

BLOCK = 256
MESH = pl.DeviceIdType.MESH
MIB = 1024 * 1024
EARLY = 5632
TILE = 512


def when(cond, fn):
    if cond is True:
        fn()
    elif cond is not False:
        pl.when(cond)(fn)


def solution(mesh):
    group = mesh.shape["col"]

    def local_product(l_cols, b_cols):
        order, local_width = l_cols.shape
        width = b_cols.shape[1]
        per_dev = local_width // BLOCK
        n_rows = order // BLOCK
        late = width - EARLY
        n_late = late // TILE
        dtype = b_cols.dtype

        def held(row, owner, t):
            low, high = group * t, group * t + group - 1
            if row >= high:
                return True
            if row < low:
                return False
            return owner + low <= row

        def late_place(k):
            return pl.ds((n_rows - 1 - k // 2) * BLOCK, BLOCK), (k % 2) * late

        def gather_kernel(l_ref, b_ref, *refs):
            x_refs, l_refs = refs[:n_rows], refs[n_rows:2 * n_rows]
            b_vmem, partial, b_sem, late_sem, own_sem, x_send, x_recv, p_send, p_recv, f_send, f_recv = refs[2 * n_rows:]
            me = lax.axis_index("col")
            across = lax.rem(me + 2, group)
            partner = me + 1 - 2 * lax.rem(me, 2)
            diagonal = lax.rem(partner + 2, group)

            barrier = pltpu.get_barrier_semaphore()
            for peer in (partner, across):
                pl.semaphore_signal(barrier, inc=1, device_id={"col": peer}, device_id_type=MESH)
            pl.semaphore_wait(barrier, 2)

            def panel(row, owner, t):
                start = pl.multiple_of((owner + group * t) * BLOCK, BLOCK)
                return l_refs[row].at[:, pl.ds(start, BLOCK)]

            def mine(row, t):
                return l_ref.at[pl.ds(row * BLOCK, BLOCK), pl.ds(t * BLOCK, BLOCK)]

            def own_copy(row, t):
                return pltpu.make_async_copy(mine(row, t), panel(row, me, t), own_sem.at[row, t])

            def send(row, t, peer, send_sem, recv_sem):
                return pltpu.make_async_remote_copy(
                    src_ref=mine(row, t), dst_ref=panel(row, me, t), send_sem=send_sem.at[row, t],
                    recv_sem=recv_sem.at[row, t], device_id={"col": peer}, device_id_type=MESH)

            def arrival(row, t, owner, recv_sem):
                dst = panel(row, owner, t)
                return pltpu.make_async_remote_copy(
                    src_ref=dst, dst_ref=dst, send_sem=x_send.at[row, t], recv_sem=recv_sem.at[row, t],
                    device_id={"col": partner}, device_id_type=MESH)

            def forward(row, t):
                block = panel(row, across, t)
                return pltpu.make_async_remote_copy(
                    src_ref=block, dst_ref=block, send_sem=f_send.at[row, t], recv_sem=f_recv.at[row, t],
                    device_id={"col": partner}, device_id_type=MESH)

            near = me - lax.rem(me, 2)
            far = 2 - near

            def load_b(k):
                rows = pl.ds(pl.multiple_of(k * BLOCK, BLOCK), BLOCK)
                return pltpu.make_async_copy(b_ref.at[rows, pl.ds(0, EARLY)], b_vmem.at[rows, :], b_sem.at[k])

            def load_late(k):
                rows, start = late_place(k)
                return pltpu.make_async_copy(
                    b_ref.at[pl.ds(k * BLOCK, BLOCK), pl.ds(EARLY, late)], b_vmem.at[rows, pl.ds(start, late)], late_sem.at[k])

            sequence = [3, 4, 5, 6, 7, 2, 1, 0]
            last = n_rows - 1
            blocks = [(row, t) for row in sequence for t in range(per_dev)]
            for row, t in blocks:
                when(held(row, me, t), lambda row=row, t=t: send(row, t, across, x_send, x_recv).start())
            for row, t in [(last, t) for t in range(per_dev)] + [b for b in blocks if b[0] != last]:
                def start_near(row=row, t=t):
                    send(row, t, partner, p_send, p_recv).start()
                    own_copy(row, t).start()
                when(held(row, me, t), start_near)
            for side in (near, far):
                for t in range(per_dev):
                    for c in range(2):
                        load_b(side + group * t + c).start()

            def relay(row):
                for t in range(per_dev):
                    def step(t=t):
                        arrival(row, t, across, x_recv).wait_recv()
                        forward(row, t).start()
                    when(held(row, across, t), step)

            def wait_near(row):
                for t in range(per_dev):
                    when(held(row, me, t), lambda t=t: own_copy(row, t).wait())
                    when(held(row, partner, t), lambda t=t: arrival(row, t, partner, p_recv).wait_recv())

            def half_product(side, start, stop):
                total = None
                for t in range(per_dev):
                    depth = pl.ds(pl.multiple_of((side + group * t) * BLOCK, 2 * BLOCK), 2 * BLOCK)
                    term = jnp.dot(l_refs[last][:, depth], b_vmem[depth, start:stop], preferred_element_type=jnp.float32)
                    total = term if total is None else total + term
                return total

            def multiply(row, start, stop):
                if row == last:
                    for n in range(start, stop, TILE):
                        total = partial[:, n:n + TILE] + half_product(far, n, n + TILE)
                        x_refs[row][:, n:n + TILE] = total.astype(dtype)
                    return
                x_refs[row][:, start:stop] = jnp.dot(
                    l_refs[row][...], b_vmem[:(row + 1) * BLOCK, start:stop],
                    preferred_element_type=jnp.float32).astype(dtype)

            wait_near(last)
            for t in range(per_dev):
                for c in range(2):
                    load_b(near + group * t + c).wait()
            middle = EARLY // (2 * TILE) * TILE
            for start in range(0, EARLY, TILE):
                if start == middle:
                    relay(sequence[0])
                partial[:, start:start + TILE] = half_product(near, start, start + TILE)
            for t in range(per_dev):
                for c in range(2):
                    load_b(far + group * t + c).wait()

            freed = []
            for place, row in enumerate(sequence):
                if row != last:
                    wait_near(row)
                for t in range(per_dev):
                    when(held(row, diagonal, t), lambda t=t: arrival(row, t, diagonal, f_recv).wait_recv())
                split = EARLY // TILE * 3 // 4 * TILE
                multiply(row, 0, split)
                if place + 1 < n_rows:
                    relay(sequence[place + 1])
                multiply(row, split, EARLY)
                free = [k for k in range(n_rows // 2, n_rows) if all(k > r for r in sequence[place + 1:])]
                for k in free:
                    if k not in freed:
                        freed.append(k)
                        for piece in range(2 * (last - k), 2 * (n_rows - k)):
                            load_late(piece).start()

            for k in range(n_rows):
                load_late(k).wait()
            for row, t in blocks:
                def drain(row=row, t=t):
                    send(row, t, across, x_send, x_recv).wait_send()
                    send(row, t, partner, p_send, p_recv).wait_send()
                when(held(row, me, t), drain)
                when(held(row, across, t), lambda row=row, t=t: forward(row, t).wait_send())

        dma = pltpu.SemaphoreType.DMA
        vmem = pl.BlockSpec(memory_space=pltpu.VMEM)
        hbm = pl.BlockSpec(memory_space=pltpu.HBM)
        gathered = pl.pallas_call(
            gather_kernel,
            out_shape=tuple(pltpu.VMEM((BLOCK, EARLY), dtype) for _ in range(n_rows))
            + tuple(pltpu.VMEM((BLOCK, BLOCK * (i + 1)), dtype) for i in range(n_rows))
            + (pltpu.VMEM((order, EARLY), dtype),),
            in_specs=[hbm, hbm],
            out_specs=(vmem,) * (2 * n_rows + 1),
            scratch_shapes=[pltpu.VMEM((BLOCK, EARLY), jnp.float32), dma((n_rows,)), dma((n_rows,))] + [dma((n_rows, per_dev))] * 7,
            compiler_params=pltpu.CompilerParams(
                collective_id=0, has_side_effects=True, vmem_limit_bytes=8 * MIB),
            name="gather_and_multiply",
        )(l_cols, b_cols)

        def finish_kernel(*refs):
            x_refs, l_refs = refs[:n_rows], refs[n_rows:2 * n_rows]
            b_vmem, out_ref, x_vmem, x_sem, early_sem = refs[2 * n_rows:]

            def put_early(row):
                return pltpu.make_async_copy(
                    x_refs[row], out_ref.at[pl.ds(row * BLOCK, BLOCK), pl.ds(0, EARLY)], early_sem.at[row])

            def put_late(n, row):
                rows = pl.ds(row * BLOCK, BLOCK)
                cols = pl.ds(pl.multiple_of(EARLY + n * TILE, TILE), TILE)
                slot = lax.rem(n, 2)
                return pltpu.make_async_copy(x_vmem.at[slot, rows, :], out_ref.at[rows, cols], x_sem.at[slot, row])

            for row in range(n_rows - 1, 4, -1):
                put_early(row).start()

            def body(n, carry):
                for row in range(5):
                    when(n == 1 + row // 2, lambda row=row: put_early(row).start())

                @pl.when(n >= 2)
                def _():
                    for row in range(n_rows):
                        put_late(n - 2, row).wait()

                for row in range(n_rows - 1, -1, -1):
                    total = None
                    for k in range(row + 1):
                        rows, start = late_place(k)
                        cols = pl.ds(pl.multiple_of(start + n * TILE, TILE), TILE)
                        term = jnp.dot(l_refs[row][:, k * BLOCK:(k + 1) * BLOCK], b_vmem[rows, cols],
                                       preferred_element_type=jnp.float32)
                        total = term if total is None else total + term
                    x_vmem[lax.rem(n, 2), pl.ds(row * BLOCK, BLOCK), :] = total.astype(dtype)
                    put_late(n, row).start()
                return carry

            lax.fori_loop(0, n_late, body, 0)
            for row in range(n_rows):
                put_early(row).wait()
            for n in range(n_late - 2, n_late):
                for row in range(n_rows):
                    put_late(n, row).wait()

        return pl.pallas_call(
            finish_kernel,
            out_shape=jax.ShapeDtypeStruct((order, width), dtype),
            in_specs=[vmem] * (2 * n_rows + 1),
            out_specs=hbm,
            scratch_shapes=[pltpu.VMEM((2, order, TILE), dtype), dma((2, n_rows)), dma((n_rows,))],
            compiler_params=pltpu.CompilerParams(vmem_limit_bytes=5 * MIB),
            name="finish",
        )(*gathered)

    return jax.shard_map(local_product, mesh=mesh, in_specs=(P("batch", "col"), P("batch", "col")), out_specs=P("batch", "col"), check_vma=False)
```

```python
import jax
import jax.numpy as jnp
from jax import lax
from jax.experimental import pallas as pl
from jax.experimental.pallas import tpu as pltpu
from jax.sharding import PartitionSpec as P

BLOCK = 256
MESH = pl.DeviceIdType.MESH
MIB = 1024 * 1024
EARLY = 5632
TILE = 512


def when(cond, fn):
    if cond is True:
        fn()
    elif cond is not False:
        pl.when(cond)(fn)


def solution(mesh):
    group = mesh.shape["col"]

    def local_product(l_cols, b_cols):
        order, local_width = l_cols.shape
        width = b_cols.shape[1]
        per_dev = local_width // BLOCK
        n_rows = order // BLOCK
        late = width - EARLY
        n_late = late // TILE
        dtype = b_cols.dtype

        def held(row, owner, t):
            low, high = group * t, group * t + group - 1
            if row >= high:
                return True
            if row < low:
                return False
            return owner + low <= row

        def late_place(k):
            return pl.ds((n_rows - 1 - k // 2) * BLOCK, BLOCK), (k % 2) * late

        def gather_kernel(l_ref, b_ref, *refs):
            x_refs, l_refs = refs[:n_rows], refs[n_rows:2 * n_rows]
            b_vmem, partial, b_sem, late_sem, own_sem, x_send, x_recv, p_send, p_recv, f_send, f_recv = refs[2 * n_rows:]
            me = lax.axis_index("col")
            across = lax.rem(me + 2, group)
            partner = me + 1 - 2 * lax.rem(me, 2)
            diagonal = lax.rem(partner + 2, group)

            def panel(row, owner, t):
                start = pl.multiple_of((owner + group * t) * BLOCK, BLOCK)
                return l_refs[row].at[:, pl.ds(start, BLOCK)]

            def mine(row, t):
                return l_ref.at[pl.ds(row * BLOCK, BLOCK), pl.ds(t * BLOCK, BLOCK)]

            def own_copy(row, t):
                return pltpu.make_async_copy(mine(row, t), panel(row, me, t), own_sem.at[row, t])

            def send(row, t, peer, send_sem, recv_sem):
                return pltpu.make_async_remote_copy(
                    src_ref=panel(row, me, t), dst_ref=panel(row, me, t), send_sem=send_sem.at[row, t],
                    recv_sem=recv_sem.at[row, t], device_id={"col": peer}, device_id_type=MESH)

            def arrival(row, t, owner, recv_sem):
                dst = panel(row, owner, t)
                return pltpu.make_async_remote_copy(
                    src_ref=dst, dst_ref=dst, send_sem=x_send.at[row, t], recv_sem=recv_sem.at[row, t],
                    device_id={"col": partner}, device_id_type=MESH)

            def forward(row, t):
                block = panel(row, across, t)
                return pltpu.make_async_remote_copy(
                    src_ref=block, dst_ref=block, send_sem=f_send.at[row, t], recv_sem=f_recv.at[row, t],
                    device_id={"col": partner}, device_id_type=MESH)

            near = me - lax.rem(me, 2)
            far = 2 - near

            def load_b(k):
                rows = pl.ds(pl.multiple_of(k * BLOCK, BLOCK), BLOCK)
                return pltpu.make_async_copy(b_ref.at[rows, pl.ds(0, EARLY)], b_vmem.at[rows, :], b_sem.at[k])

            def load_late(k):
                rows, start = late_place(k)
                return pltpu.make_async_copy(
                    b_ref.at[pl.ds(k * BLOCK, BLOCK), pl.ds(EARLY, late)], b_vmem.at[rows, pl.ds(start, late)], late_sem.at[k])

            sequence = [3, 4, 5, 6, 7, 2, 1, 0]
            last = n_rows - 1
            blocks = [(row, t) for row in sequence for t in range(per_dev)]
            barrier = pltpu.get_barrier_semaphore()
            for peer in (partner, across):
                pl.semaphore_signal(barrier, inc=1, device_id={"col": peer}, device_id_type=MESH)
            for row, t in blocks:
                when(held(row, me, t), lambda row=row, t=t: own_copy(row, t).start())
            for side in (near, far):
                for t in range(per_dev):
                    for c in range(2):
                        load_b(side + group * t + c).start()

            pl.semaphore_wait(barrier, 2)

            for row, t in blocks:
                def start_across(row=row, t=t):
                    own_copy(row, t).wait()
                    send(row, t, across, x_send, x_recv).start()
                when(held(row, me, t), start_across)
            for row, t in [(last, t) for t in range(per_dev)] + [b for b in blocks if b[0] != last]:
                when(held(row, me, t), lambda row=row, t=t: send(row, t, partner, p_send, p_recv).start())

            def relay(row):
                for t in range(per_dev):
                    def step(t=t):
                        arrival(row, t, across, x_recv).wait_recv()
                        forward(row, t).start()
                    when(held(row, across, t), step)

            def wait_near(row):
                for t in range(per_dev):
                    when(held(row, partner, t), lambda t=t: arrival(row, t, partner, p_recv).wait_recv())

            def half_product(side, start, stop):
                total = None
                for t in range(per_dev):
                    depth = pl.ds(pl.multiple_of((side + group * t) * BLOCK, 2 * BLOCK), 2 * BLOCK)
                    term = jnp.dot(l_refs[last][:, depth], b_vmem[depth, start:stop], preferred_element_type=jnp.float32)
                    total = term if total is None else total + term
                return total

            def multiply(row, start, stop):
                if row == last:
                    for n in range(start, stop, TILE):
                        total = partial[:, n:n + TILE] + half_product(far, n, n + TILE)
                        x_refs[row][:, n:n + TILE] = total.astype(dtype)
                    return
                x_refs[row][:, start:stop] = jnp.dot(
                    l_refs[row][...], b_vmem[:(row + 1) * BLOCK, start:stop],
                    preferred_element_type=jnp.float32).astype(dtype)

            wait_near(last)
            for t in range(per_dev):
                for c in range(2):
                    load_b(near + group * t + c).wait()
            middle = EARLY // (2 * TILE) * TILE
            for start in range(0, EARLY, TILE):
                if start == middle:
                    relay(sequence[0])
                partial[:, start:start + TILE] = half_product(near, start, start + TILE)
            for t in range(per_dev):
                for c in range(2):
                    load_b(far + group * t + c).wait()

            freed = []
            for place, row in enumerate(sequence):
                if row != last:
                    wait_near(row)
                for t in range(per_dev):
                    when(held(row, diagonal, t), lambda t=t: arrival(row, t, diagonal, f_recv).wait_recv())
                split = EARLY // TILE * 3 // 4 * TILE
                multiply(row, 0, split)
                if place + 1 < n_rows:
                    relay(sequence[place + 1])
                multiply(row, split, EARLY)
                free = [k for k in range(n_rows // 2, n_rows) if all(k > r for r in sequence[place + 1:])]
                for k in free:
                    if k not in freed:
                        freed.append(k)
                        for piece in range(2 * (last - k), 2 * (n_rows - k)):
                            load_late(piece).start()

            for k in range(n_rows):
                load_late(k).wait()
            for row, t in blocks:
                def drain(row=row, t=t):
                    send(row, t, across, x_send, x_recv).wait_send()
                    send(row, t, partner, p_send, p_recv).wait_send()
                when(held(row, me, t), drain)
                when(held(row, across, t), lambda row=row, t=t: forward(row, t).wait_send())

        dma = pltpu.SemaphoreType.DMA
        vmem = pl.BlockSpec(memory_space=pltpu.VMEM)
        hbm = pl.BlockSpec(memory_space=pltpu.HBM)
        gathered = pl.pallas_call(
            gather_kernel,
            out_shape=tuple(pltpu.VMEM((BLOCK, EARLY), dtype) for _ in range(n_rows))
            + tuple(pltpu.VMEM((BLOCK, BLOCK * (i + 1)), dtype) for i in range(n_rows))
            + (pltpu.VMEM((order, EARLY), dtype),),
            in_specs=[hbm, hbm],
            out_specs=(vmem,) * (2 * n_rows + 1),
            scratch_shapes=[pltpu.VMEM((BLOCK, EARLY), jnp.float32), dma((n_rows,)), dma((n_rows,))] + [dma((n_rows, per_dev))] * 7,
            compiler_params=pltpu.CompilerParams(
                collective_id=0, has_side_effects=True, vmem_limit_bytes=8 * MIB),
            name="gather_and_multiply",
        )(l_cols, b_cols)

        def finish_kernel(*refs):
            x_refs, l_refs = refs[:n_rows], refs[n_rows:2 * n_rows]
            b_vmem, out_ref, x_vmem, x_sem, early_sem = refs[2 * n_rows:]

            def put_early(row):
                return pltpu.make_async_copy(
                    x_refs[row], out_ref.at[pl.ds(row * BLOCK, BLOCK), pl.ds(0, EARLY)], early_sem.at[row])

            def put_late(n, row):
                rows = pl.ds(row * BLOCK, BLOCK)
                cols = pl.ds(pl.multiple_of(EARLY + n * TILE, TILE), TILE)
                slot = lax.rem(n, 2)
                return pltpu.make_async_copy(x_vmem.at[slot, rows, :], out_ref.at[rows, cols], x_sem.at[slot, row])

            for row in range(n_rows - 1, 4, -1):
                put_early(row).start()

            def body(n, carry):
                for row in range(5):
                    when(n == 1 + row // 2, lambda row=row: put_early(row).start())

                @pl.when(n >= 2)
                def _():
                    for row in range(n_rows):
                        put_late(n - 2, row).wait()

                for row in range(n_rows - 1, -1, -1):
                    total = None
                    for k in range(row + 1):
                        rows, start = late_place(k)
                        cols = pl.ds(pl.multiple_of(start + n * TILE, TILE), TILE)
                        term = jnp.dot(l_refs[row][:, k * BLOCK:(k + 1) * BLOCK], b_vmem[rows, cols],
                                       preferred_element_type=jnp.float32)
                        total = term if total is None else total + term
                    x_vmem[lax.rem(n, 2), pl.ds(row * BLOCK, BLOCK), :] = total.astype(dtype)
                    put_late(n, row).start()
                return carry

            lax.fori_loop(0, n_late, body, 0)
            for row in range(n_rows):
                put_early(row).wait()
            for n in range(n_late - 2, n_late):
                for row in range(n_rows):
                    put_late(n, row).wait()

        return pl.pallas_call(
            finish_kernel,
            out_shape=jax.ShapeDtypeStruct((order, width), dtype),
            in_specs=[vmem] * (2 * n_rows + 1),
            out_specs=hbm,
            scratch_shapes=[pltpu.VMEM((2, order, TILE), dtype), dma((2, n_rows)), dma((n_rows,))],
            compiler_params=pltpu.CompilerParams(vmem_limit_bytes=5 * MIB),
            name="finish",
        )(*gathered)

    return jax.shard_map(local_product, mesh=mesh, in_specs=(P("batch", "col"), P("batch", "col")), out_specs=P("batch", "col"), check_vma=False)
```

```python
import jax
import jax.numpy as jnp
from jax import lax
from jax.experimental import pallas as pl
from jax.experimental.pallas import tpu as pltpu
from jax.sharding import PartitionSpec as P

BLOCK = 256
MESH = pl.DeviceIdType.MESH
MIB = 1024 * 1024
EARLY = 5632
TILE = 512


def when(cond, fn):
    if cond is True:
        fn()
    elif cond is not False:
        pl.when(cond)(fn)


def solution(mesh):
    group = mesh.shape["col"]

    def local_product(l_cols, b_cols):
        order, local_width = l_cols.shape
        width = b_cols.shape[1]
        per_dev = local_width // BLOCK
        n_rows = order // BLOCK
        late = width - EARLY
        n_late = late // TILE
        dtype = b_cols.dtype

        def held(row, owner, t):
            low, high = group * t, group * t + group - 1
            if row >= high:
                return True
            if row < low:
                return False
            return owner + low <= row

        def pieces(row, t, owner):
            full = [(0, BLOCK, BLOCK)]
            high = row - group * t
            if high >= group:
                return [(True, full)]
            if high < 0:
                return []
            half = BLOCK // 2
            cases = [(owner == high, [(0, half, half), (half, half, BLOCK)])]
            if high > 0:
                cases.append((owner < high, full))
            return cases

        def late_place(k):
            return pl.ds((n_rows - 1 - k // 2) * BLOCK, BLOCK), (k % 2) * late

        def gather_kernel(l_ref, b_ref, *refs):
            x_refs, l_refs = refs[:n_rows], refs[n_rows:2 * n_rows]
            b_vmem, partial, b_sem, late_sem, own_sem, p_send, p_recv, x_send, x_recv, f_send, f_recv = refs[2 * n_rows:]
            me = lax.axis_index("col")
            across = lax.rem(me + 2, group)
            partner = me + 1 - 2 * lax.rem(me, 2)
            diagonal = lax.rem(partner + 2, group)

            def panel(row, owner, t):
                start = pl.multiple_of((owner + group * t) * BLOCK, BLOCK)
                return l_refs[row].at[:, pl.ds(start, BLOCK)]

            def mine(row, t):
                return l_ref.at[pl.ds(row * BLOCK, BLOCK), pl.ds(t * BLOCK, BLOCK)]

            def own_copy(row, t):
                return pltpu.make_async_copy(mine(row, t), panel(row, me, t), own_sem.at[row, t])

            def remote(src, dst, send_sem, recv_sem, peer):
                return pltpu.make_async_remote_copy(
                    src_ref=src, dst_ref=dst, send_sem=send_sem, recv_sem=recv_sem, device_id={"col": peer}, device_id_type=MESH)

            def share(row, t, owner):
                block = panel(row, owner, t)
                return remote(block, block, p_send.at[row, t], p_recv.at[row, t], partner)

            def parts(row, t, owner, send_sem, recv_sem, peer, act):
                for cond, rects in pieces(row, t, owner):
                    def run(rects=rects):
                        for j, (first, rows, width) in enumerate(rects):
                            start = pl.multiple_of((owner + group * t) * BLOCK, BLOCK)
                            part = l_refs[row].at[pl.ds(first, rows), pl.ds(start, width)]
                            act(j, remote(part, part, send_sem.at[row, t, j], recv_sem.at[row, t, j], peer))
                    when(cond, run)

            def parts_both(row, t, owner, act):
                for cond, rects in pieces(row, t, owner):
                    def run(rects=rects):
                        for j, (first, rows, width) in enumerate(rects):
                            start = pl.multiple_of((owner + group * t) * BLOCK, BLOCK)
                            part = l_refs[row].at[pl.ds(first, rows), pl.ds(start, width)]
                            act(remote(part, part, x_send.at[row, t, j], x_recv.at[row, t, j], across),
                                remote(part, part, f_send.at[row, t, j], f_recv.at[row, t, j], partner))
                    when(cond, run)

            near = me - lax.rem(me, 2)
            far = 2 - near

            def load_b(k):
                rows = pl.ds(pl.multiple_of(k * BLOCK, BLOCK), BLOCK)
                return pltpu.make_async_copy(b_ref.at[rows, pl.ds(0, EARLY)], b_vmem.at[rows, :], b_sem.at[k])

            def load_late(k):
                rows, start = late_place(k)
                return pltpu.make_async_copy(
                    b_ref.at[pl.ds(k * BLOCK, BLOCK), pl.ds(EARLY, late)], b_vmem.at[rows, pl.ds(start, late)], late_sem.at[k])

            sequence = [3, 6, 5, 4, 7, 2, 1, 0]
            before = [8, 8, 8, 8, 5, 5, 0, 0]
            last = n_rows - 1
            blocks = [(row, t) for row in sequence for t in range(per_dev)]
            shared = [(last, t) for t in range(per_dev)] + [b for b in blocks if b[0] != last]

            barrier = pltpu.get_barrier_semaphore()
            for peer in (partner, across):
                pl.semaphore_signal(barrier, inc=1, device_id={"col": peer}, device_id_type=MESH)
            for row, t in shared:
                when(held(row, me, t), lambda row=row, t=t: own_copy(row, t).start())
            for row in range(n_rows):
                def clear(row=row):
                    l_refs[row][:BLOCK // 2, row * BLOCK + BLOCK // 2:] = jnp.zeros((BLOCK // 2, BLOCK // 2), dtype)
                when(far == row % group // 2 * 2, clear)
            for row, t in shared:
                when(held(row, me, t), lambda row=row, t=t: own_copy(row, t).wait())
            for side in (near, far):
                for t in range(per_dev):
                    for c in range(2):
                        load_b(side + group * t + c).start()
            pl.semaphore_wait(barrier, 2)

            for row, t in blocks:
                parts(row, t, me, x_send, x_recv, across, lambda j, copy: copy.start())
            for row, t in shared:
                when(held(row, me, t), lambda row=row, t=t: share(row, t, me).start())

            def relay(row):
                def step(came, on):
                    came.wait_recv()
                    on.start()
                for t in range(per_dev):
                    parts_both(row, t, across, step)

            def wait_near(row):
                for t in range(per_dev):
                    when(held(row, partner, t), lambda t=t: share(row, t, partner).wait_recv())

            def half_product(side, start, stop):
                total = None
                for t in range(per_dev):
                    depth = pl.ds(pl.multiple_of((side + group * t) * BLOCK, 2 * BLOCK), 2 * BLOCK)
                    term = jnp.dot(l_refs[last][:, depth], b_vmem[depth, start:stop], preferred_element_type=jnp.float32)
                    total = term if total is None else total + term
                return total

            def multiply(row, start, stop):
                if row == last:
                    for n in range(start, stop, TILE):
                        total = partial[:, n:n + TILE] + half_product(far, n, n + TILE)
                        x_refs[row][:, n:n + TILE] = total.astype(dtype)
                    return
                x_refs[row][:, start:stop] = jnp.dot(
                    l_refs[row][...], b_vmem[:(row + 1) * BLOCK, start:stop],
                    preferred_element_type=jnp.float32).astype(dtype)

            wait_near(last)
            for t in range(per_dev):
                for c in range(2):
                    load_b(near + group * t + c).wait()
            middle = EARLY // (2 * TILE) * TILE
            for start in range(0, EARLY, TILE):
                if start == middle:
                    relay(sequence[0])
                partial[:, start:start + TILE] = half_product(near, start, start + TILE)
            for t in range(per_dev):
                for c in range(2):
                    load_b(far + group * t + c).wait()

            freed = []
            for place, row in enumerate(sequence):
                if row != last:
                    wait_near(row)
                for t in range(per_dev):
                    parts(row, t, diagonal, f_send, f_recv, partner, lambda j, copy: copy.wait_recv())
                split = before[place] * TILE
                if split:
                    multiply(row, 0, split)
                if place + 1 < n_rows:
                    relay(sequence[place + 1])
                multiply(row, split, EARLY)
                free = [k for k in range(n_rows // 2, n_rows) if all(k > r for r in sequence[place + 1:])]
                for k in free:
                    if k not in freed:
                        freed.append(k)
                        for piece in range(2 * (last - k), 2 * (n_rows - k)):
                            load_late(piece).start()

            for k in range(n_rows):
                load_late(k).wait()
            for row, t in blocks:
                parts(row, t, me, x_send, x_recv, across, lambda j, copy: copy.wait_send())
                when(held(row, me, t), lambda row=row, t=t: share(row, t, me).wait_send())
                parts(row, t, across, f_send, f_recv, partner, lambda j, copy: copy.wait_send())

        dma = pltpu.SemaphoreType.DMA
        vmem = pl.BlockSpec(memory_space=pltpu.VMEM)
        hbm = pl.BlockSpec(memory_space=pltpu.HBM)
        gathered = pl.pallas_call(
            gather_kernel,
            out_shape=tuple(pltpu.VMEM((BLOCK, EARLY), dtype) for _ in range(n_rows))
            + tuple(pltpu.VMEM((BLOCK, BLOCK * (i + 1)), dtype) for i in range(n_rows))
            + (pltpu.VMEM((order, EARLY), dtype),),
            in_specs=[hbm, hbm],
            out_specs=(vmem,) * (2 * n_rows + 1),
            scratch_shapes=[pltpu.VMEM((BLOCK, EARLY), jnp.float32), dma((n_rows,)), dma((n_rows,))]
            + [dma((n_rows, per_dev))] * 3 + [dma((n_rows, per_dev, 2))] * 4,
            compiler_params=pltpu.CompilerParams(
                collective_id=0, has_side_effects=True, vmem_limit_bytes=8 * MIB),
            name="gather_and_multiply",
        )(l_cols, b_cols)

        def finish_kernel(*refs):
            x_refs, l_refs = refs[:n_rows], refs[n_rows:2 * n_rows]
            b_vmem, out_ref, x_vmem, x_sem, early_sem = refs[2 * n_rows:]

            def put_early(row):
                return pltpu.make_async_copy(
                    x_refs[row], out_ref.at[pl.ds(row * BLOCK, BLOCK), pl.ds(0, EARLY)], early_sem.at[row])

            def put_late(n, row):
                rows = pl.ds(row * BLOCK, BLOCK)
                cols = pl.ds(EARLY + n * TILE, TILE)
                slot = n % 2
                return pltpu.make_async_copy(x_vmem.at[slot, rows, :], out_ref.at[rows, cols], x_sem.at[slot, row])

            for row in range(n_rows - 1, 4, -1):
                put_early(row).start()

            for n in range(n_late):
                for row in range(5):
                    if n == 1 + row // 2:
                        put_early(row).start()
                if n >= 2:
                    for row in range(n_rows):
                        put_late(n - 2, row).wait()
                for row in range(n_rows - 1, -1, -1):
                    total = None
                    for k in range(row + 1):
                        rows, start = late_place(k)
                        term = jnp.dot(l_refs[row][:, k * BLOCK:(k + 1) * BLOCK],
                                       b_vmem[rows, start + n * TILE:start + (n + 1) * TILE],
                                       preferred_element_type=jnp.float32)
                        total = term if total is None else total + term
                    x_vmem[n % 2, row * BLOCK:(row + 1) * BLOCK, :] = total.astype(dtype)
                    put_late(n, row).start()

            for row in range(n_rows):
                put_early(row).wait()
            for n in range(n_late - 2, n_late):
                for row in range(n_rows):
                    put_late(n, row).wait()

        return pl.pallas_call(
            finish_kernel,
            out_shape=jax.ShapeDtypeStruct((order, width), dtype),
            in_specs=[vmem] * (2 * n_rows + 1),
            out_specs=hbm,
            scratch_shapes=[pltpu.VMEM((2, order, TILE), dtype), dma((2, n_rows)), dma((n_rows,))],
            compiler_params=pltpu.CompilerParams(vmem_limit_bytes=5 * MIB),
            name="finish",
        )(*gathered)

    return jax.shard_map(local_product, mesh=mesh, in_specs=(P("batch", "col"), P("batch", "col")), out_specs=P("batch", "col"), check_vma=False)
```

```python
import jax
import jax.numpy as jnp
from jax import lax
from jax.experimental import pallas as pl
from jax.experimental.pallas import tpu as pltpu
from jax.sharding import PartitionSpec as P

BLOCK = 256
MESH = pl.DeviceIdType.MESH
MIB = 1024 * 1024
EARLY = 5632
TILE = 512


def when(cond, fn):
    if cond is True:
        fn()
    elif cond is not False:
        pl.when(cond)(fn)


def solution(mesh):
    group = mesh.shape["col"]

    def local_product(l_cols, b_cols):
        order, local_width = l_cols.shape
        width = b_cols.shape[1]
        per_dev = local_width // BLOCK
        n_rows = order // BLOCK
        late = width - EARLY
        n_late = late // TILE
        dtype = b_cols.dtype

        def held(row, owner, t):
            low, high = group * t, group * t + group - 1
            if row >= high:
                return True
            if row < low:
                return False
            return owner + low <= row

        def pieces(row, t, owner):
            full = [(0, BLOCK, BLOCK)]
            high = row - group * t
            if high >= group:
                return [(True, full)]
            if high < 0:
                return []
            half = BLOCK // 2
            cases = [(owner == high, [(0, half, half), (half, half, BLOCK)])]
            if high > 0:
                cases.append((owner < high, full))
            return cases

        def chip_sides():
            me = lax.axis_index("col")
            near = me - lax.rem(me, 2)
            return near, 2 - near

        def late_place(k):
            block = chip_sides()[k // group] + group + k % group // 2
            return pl.ds(pl.multiple_of(block * BLOCK, BLOCK), BLOCK), k % 2 * late

        def gather_kernel(l_ref, b_ref, *refs):
            x_refs, l_refs = refs[:n_rows], refs[n_rows:2 * n_rows]
            b_vmem, partial, b_sem, late_sem, own_sem, p_send, p_recv, x_send, x_recv, f_send, f_recv = refs[2 * n_rows:]
            me = lax.axis_index("col")
            across = lax.rem(me + 2, group)
            partner = me + 1 - 2 * lax.rem(me, 2)
            diagonal = lax.rem(partner + 2, group)

            def panel(row, owner, t):
                start = pl.multiple_of((owner + group * t) * BLOCK, BLOCK)
                return l_refs[row].at[:, pl.ds(start, BLOCK)]

            def mine(row, t):
                return l_ref.at[pl.ds(row * BLOCK, BLOCK), pl.ds(t * BLOCK, BLOCK)]

            def own_copy(row, t):
                return pltpu.make_async_copy(mine(row, t), panel(row, me, t), own_sem.at[row, t])

            def remote(src, dst, send_sem, recv_sem, peer):
                return pltpu.make_async_remote_copy(
                    src_ref=src, dst_ref=dst, send_sem=send_sem, recv_sem=recv_sem, device_id={"col": peer}, device_id_type=MESH)

            def share(row, t, owner):
                block = panel(row, owner, t)
                return remote(block, block, p_send.at[row, t], p_recv.at[row, t], partner)

            def parts(row, t, owner, send_sem, recv_sem, peer, act):
                for cond, rects in pieces(row, t, owner):
                    def run(rects=rects):
                        for j, (first, rows, width) in enumerate(rects):
                            start = pl.multiple_of((owner + group * t) * BLOCK, BLOCK)
                            part = l_refs[row].at[pl.ds(first, rows), pl.ds(start, width)]
                            act(j, remote(part, part, send_sem.at[row, t, j], recv_sem.at[row, t, j], peer))
                    when(cond, run)

            def parts_both(row, t, owner, act):
                for cond, rects in pieces(row, t, owner):
                    def run(rects=rects):
                        for j, (first, rows, width) in enumerate(rects):
                            start = pl.multiple_of((owner + group * t) * BLOCK, BLOCK)
                            part = l_refs[row].at[pl.ds(first, rows), pl.ds(start, width)]
                            act(remote(part, part, x_send.at[row, t, j], x_recv.at[row, t, j], across),
                                remote(part, part, f_send.at[row, t, j], f_recv.at[row, t, j], partner))
                    when(cond, run)

            near, far = chip_sides()

            def load_b(k):
                rows = pl.ds(pl.multiple_of(k * BLOCK, BLOCK), BLOCK)
                return pltpu.make_async_copy(b_ref.at[rows, pl.ds(0, EARLY)], b_vmem.at[rows, :], b_sem.at[k])

            def load_late(k):
                rows, start = late_place(k)
                return pltpu.make_async_copy(
                    b_ref.at[pl.ds(k * BLOCK, BLOCK), pl.ds(EARLY, late)], b_vmem.at[rows, pl.ds(start, late)], late_sem.at[k])

            sequence = [3, 6, 5, 4, 7, 2, 1, 0]
            before = [8, 8, 8, 8, 5, 5, 0, 0]
            last = n_rows - 1
            blocks = [(row, t) for row in sequence for t in range(per_dev)]
            shared = [(last, t) for t in range(per_dev)] + [b for b in blocks if b[0] != last]

            barrier = pltpu.get_barrier_semaphore()
            for peer in (partner, across):
                pl.semaphore_signal(barrier, inc=1, device_id={"col": peer}, device_id_type=MESH)
            for row, t in shared:
                when(held(row, me, t), lambda row=row, t=t: own_copy(row, t).start())
            for row in range(n_rows):
                def clear(row=row):
                    l_refs[row][:BLOCK // 2, row * BLOCK + BLOCK // 2:] = jnp.zeros((BLOCK // 2, BLOCK // 2), dtype)
                when(far == row % group // 2 * 2, clear)
            for row, t in shared:
                when(held(row, me, t), lambda row=row, t=t: own_copy(row, t).wait())
            for side in (near, far):
                for t in range(per_dev):
                    for c in range(2):
                        load_b(side + group * t + c).start()
            pl.semaphore_wait(barrier, 2)

            for row, t in blocks:
                parts(row, t, me, x_send, x_recv, across, lambda j, copy: copy.start())
            for row, t in shared:
                when(held(row, me, t), lambda row=row, t=t: share(row, t, me).start())

            def relay(row):
                def step(came, on):
                    came.wait_recv()
                    on.start()
                for t in range(per_dev):
                    parts_both(row, t, across, step)

            def wait_near(row):
                for t in range(per_dev):
                    when(held(row, partner, t), lambda t=t: share(row, t, partner).wait_recv())

            def half_product(side, start, stop):
                total = None
                for t in range(per_dev):
                    depth = pl.ds(pl.multiple_of((side + group * t) * BLOCK, 2 * BLOCK), 2 * BLOCK)
                    term = jnp.dot(l_refs[last][:, depth], b_vmem[depth, start:stop], preferred_element_type=jnp.float32)
                    total = term if total is None else total + term
                return total

            def multiply(row, start, stop):
                if row == last:
                    for n in range(start, stop, TILE):
                        total = partial[:, n:n + TILE] + half_product(far, n, n + TILE)
                        x_refs[row][:, n:n + TILE] = total.astype(dtype)
                    return
                x_refs[row][:, start:stop] = jnp.dot(
                    l_refs[row][...], b_vmem[:(row + 1) * BLOCK, start:stop],
                    preferred_element_type=jnp.float32).astype(dtype)

            wait_near(last)
            for t in range(per_dev):
                for c in range(2):
                    load_b(near + group * t + c).wait()
            middle = EARLY // (2 * TILE) * TILE
            for start in range(0, EARLY, TILE):
                if start == middle:
                    relay(sequence[0])
                partial[:, start:start + TILE] = half_product(near, start, start + TILE)
            for t in range(per_dev):
                for c in range(2):
                    load_b(far + group * t + c).wait()

            for place, row in enumerate(sequence):
                if row != last:
                    wait_near(row)
                for t in range(per_dev):
                    parts(row, t, diagonal, f_send, f_recv, partner, lambda j, copy: copy.wait_recv())
                split = before[place] * TILE
                if split:
                    multiply(row, 0, split)
                if place + 1 < n_rows:
                    relay(sequence[place + 1])
                multiply(row, split, EARLY)
                if row == 4:
                    for k in range(group):
                        load_late(k).start()
                if row == last:
                    for k in range(group, n_rows):
                        load_late(k).start()

            for k in range(n_rows):
                load_late(k).wait()
            for row, t in blocks:
                parts(row, t, me, x_send, x_recv, across, lambda j, copy: copy.wait_send())
                when(held(row, me, t), lambda row=row, t=t: share(row, t, me).wait_send())
                parts(row, t, across, f_send, f_recv, partner, lambda j, copy: copy.wait_send())

        dma = pltpu.SemaphoreType.DMA
        vmem = pl.BlockSpec(memory_space=pltpu.VMEM)
        hbm = pl.BlockSpec(memory_space=pltpu.HBM)
        gathered = pl.pallas_call(
            gather_kernel,
            out_shape=tuple(pltpu.VMEM((BLOCK, EARLY), dtype) for _ in range(n_rows))
            + tuple(pltpu.VMEM((BLOCK, BLOCK * (i + 1)), dtype) for i in range(n_rows))
            + (pltpu.VMEM((order, EARLY), dtype),),
            in_specs=[hbm, hbm],
            out_specs=(vmem,) * (2 * n_rows + 1),
            scratch_shapes=[pltpu.VMEM((BLOCK, EARLY), jnp.float32), dma((n_rows,)), dma((n_rows,))]
            + [dma((n_rows, per_dev))] * 3 + [dma((n_rows, per_dev, 2))] * 4,
            compiler_params=pltpu.CompilerParams(
                collective_id=0, has_side_effects=True, vmem_limit_bytes=8 * MIB),
            name="gather_and_multiply",
        )(l_cols, b_cols)

        def finish_kernel(*refs):
            x_refs, l_refs = refs[:n_rows], refs[n_rows:2 * n_rows]
            b_vmem, out_ref, x_late, late_sem, early_sem = refs[2 * n_rows:]

            def put_early(row):
                return pltpu.make_async_copy(
                    x_refs[row], out_ref.at[pl.ds(row * BLOCK, BLOCK), pl.ds(0, EARLY)], early_sem.at[row])

            def place(row):
                return pl.ds(row // 2 * BLOCK, BLOCK), row % 2 * late

            def tile(start, n):
                return pl.ds(pl.multiple_of(start + n * TILE, TILE), TILE)

            def put_late(row, n):
                rows, start = place(row)
                return pltpu.make_async_copy(
                    x_late.at[rows, tile(start, n)], out_ref.at[pl.ds(row * BLOCK, BLOCK), tile(EARLY, n)], late_sem.at[n, row])

            for row in range(n_rows - 1, -1, -1):
                put_early(row).start()
            def body(n, carry):
                for row in range(n_rows - 1, -1, -1):
                    total = None
                    for k in range(row + 1):
                        rows, start = late_place(k)
                        term = jnp.dot(l_refs[row][:, k * BLOCK:(k + 1) * BLOCK], b_vmem[rows, tile(start, n)],
                                       preferred_element_type=jnp.float32)
                        total = term if total is None else total + term
                    rows, start = place(row)
                    x_late[rows, tile(start, n)] = total.astype(dtype)
                for row in range(n_rows - 1, -1, -1):
                    put_late(row, n).start()
                return carry

            lax.fori_loop(0, n_late, body, 0)
            for row in range(n_rows - 1, -1, -1):
                put_early(row).wait()
                for n in range(n_late):
                    put_late(row, n).wait()

        return pl.pallas_call(
            finish_kernel,
            out_shape=(jax.ShapeDtypeStruct((order, width), dtype), pltpu.VMEM((order, EARLY), dtype)),
            in_specs=[vmem] * (2 * n_rows + 1),
            out_specs=(hbm, vmem),
            input_output_aliases={2 * n_rows: 1},
            scratch_shapes=[dma((n_late, n_rows)), dma((n_rows,))],
            compiler_params=pltpu.CompilerParams(vmem_limit_bytes=5 * MIB),
            name="finish",
        )(*gathered)[0]

    return jax.shard_map(local_product, mesh=mesh, in_specs=(P("batch", "col"), P("batch", "col")), out_specs=P("batch", "col"), check_vma=False)
```

```python
import jax
import jax.numpy as jnp
from jax import lax
from jax.experimental import pallas as pl
from jax.experimental.pallas import tpu as pltpu
from jax.sharding import PartitionSpec as P

BLOCK = 256
MESH = pl.DeviceIdType.MESH
MIB = 1024 * 1024
EARLY = 5632
TILE = 512


def when(cond, fn):
    if cond is True:
        fn()
    elif cond is not False:
        pl.when(cond)(fn)


def solution(mesh):
    group = mesh.shape["col"]

    def local_product(l_cols, b_cols):
        order, local_width = l_cols.shape
        width = b_cols.shape[1]
        per_dev = local_width // BLOCK
        n_rows = order // BLOCK
        late = width - EARLY
        n_late = late // TILE
        dtype = b_cols.dtype

        def held(row, owner, t):
            low, high = group * t, group * t + group - 1
            if row >= high:
                return True
            if row < low:
                return False
            return owner + low <= row

        def pieces(row, t, owner):
            full = [(0, BLOCK, BLOCK)]
            high = row - group * t
            if high >= group:
                return [(True, full)]
            if high < 0:
                return []
            half = BLOCK // 2
            cases = [(owner == high, [(0, half, half), (half, half, BLOCK)])]
            if high > 0:
                cases.append((owner < high, full))
            return cases

        def late_place(k):
            return pl.ds((n_rows - 1 - k // 2) * BLOCK, BLOCK), (k % 2) * late

        def gather_kernel(l_ref, b_ref, *refs):
            x_refs, l_refs = refs[:n_rows], refs[n_rows:2 * n_rows]
            b_vmem, partial, b_sem, late_sem, own_sem, p_send, p_recv, x_send, x_recv, f_send, f_recv = refs[2 * n_rows:]
            me = lax.axis_index("col")
            across = lax.rem(me + 2, group)
            partner = me + 1 - 2 * lax.rem(me, 2)
            diagonal = lax.rem(partner + 2, group)

            def panel(row, owner, t):
                start = pl.multiple_of((owner + group * t) * BLOCK, BLOCK)
                return l_refs[row].at[:, pl.ds(start, BLOCK)]

            def mine(row, t):
                return l_ref.at[pl.ds(row * BLOCK, BLOCK), pl.ds(t * BLOCK, BLOCK)]

            def own_copy(row, t):
                return pltpu.make_async_copy(mine(row, t), panel(row, me, t), own_sem)

            def slot(row, t, part=0):
                if part:
                    return 2 * n_rows - group + row
                return row if t == 0 else n_rows - group + row

            def wait_all(sem, owner, halves):
                for c in range(group):
                    width = (2 * n_rows - group - 2 * c) * BLOCK - (BLOCK // 2 if halves else 0)
                    like = x_refs[last].at[:, pl.ds(0, width)]
                    pl.when(owner == c)(lambda like=like: pltpu.make_async_copy(like, like, sem).wait())

            last = n_rows - 1

            def remote(src, dst, send_sem, recv_sem, peer):
                return pltpu.make_async_remote_copy(
                    src_ref=src, dst_ref=dst, send_sem=send_sem, recv_sem=recv_sem, device_id={"col": peer}, device_id_type=MESH)

            def share(row, t, owner):
                block = panel(row, owner, t)
                return remote(block, block, p_send, p_recv.at[slot(row, t)], partner)

            def parts(row, t, owner, send_sem, recv_sem, peer, act):
                for cond, rects in pieces(row, t, owner):
                    def run(rects=rects):
                        for j, (first, rows, width) in enumerate(rects):
                            start = pl.multiple_of((owner + group * t) * BLOCK, BLOCK)
                            part = l_refs[row].at[pl.ds(first, rows), pl.ds(start, width)]
                            act(j, remote(part, part, send_sem, recv_sem.at[slot(row, t, j)], peer))
                    when(cond, run)

            def parts_both(row, t, owner, act):
                for cond, rects in pieces(row, t, owner):
                    def run(rects=rects):
                        for j, (first, rows, width) in enumerate(rects):
                            start = pl.multiple_of((owner + group * t) * BLOCK, BLOCK)
                            part = l_refs[row].at[pl.ds(first, rows), pl.ds(start, width)]
                            act(remote(part, part, x_send, x_recv.at[slot(row, t, j)], across),
                                remote(part, part, f_send, f_recv.at[slot(row, t, j)], partner))
                    when(cond, run)

            near = me - lax.rem(me, 2)
            far = 2 - near

            def load_b(k, sem):
                rows = pl.ds(pl.multiple_of(k * BLOCK, BLOCK), BLOCK)
                return pltpu.make_async_copy(b_ref.at[rows, pl.ds(0, EARLY)], b_vmem.at[rows, :], sem)

            def wait_side(i):
                like = b_vmem.at[pl.ds(0, n_rows // 2 * BLOCK), :]
                pltpu.make_async_copy(like, like, b_sem.at[i]).wait()

            def load_late(k):
                rows, start = late_place(k)
                return pltpu.make_async_copy(
                    b_ref.at[pl.ds(k * BLOCK, BLOCK), pl.ds(EARLY, late)], b_vmem.at[rows, pl.ds(start, late)], late_sem)

            sequence = [3, 6, 5, 4, 7, 2, 1, 0]
            before = [8, 8, 8, 8, 5, 5, 0, 0]
            blocks = [(row, t) for row in sequence for t in range(per_dev)]
            shared = [(last, t) for t in range(per_dev)] + [b for b in blocks if b[0] != last]

            barrier = pltpu.get_barrier_semaphore()
            for peer in (partner, across):
                pl.semaphore_signal(barrier, inc=1, device_id={"col": peer}, device_id_type=MESH)
            for row, t in shared:
                when(held(row, me, t), lambda row=row, t=t: own_copy(row, t).start())
            for row in range(n_rows):
                def clear(row=row):
                    l_refs[row][:BLOCK // 2, row * BLOCK + BLOCK // 2:] = jnp.zeros((BLOCK // 2, BLOCK // 2), dtype)
                when(far == row % group // 2 * 2, clear)
            wait_all(own_sem, me, False)
            for i, side in enumerate((near, far)):
                for t in range(per_dev):
                    for c in range(2):
                        load_b(side + group * t + c, b_sem.at[i]).start()
            pl.semaphore_wait(barrier, 2)

            for row, t in blocks:
                parts(row, t, me, x_send, x_recv, across, lambda j, copy: copy.start())
            for row, t in shared:
                when(held(row, me, t), lambda row=row, t=t: share(row, t, me).start())

            def relay(row):
                def step(came, on):
                    came.wait_recv()
                    on.start()
                for t in range(per_dev):
                    parts_both(row, t, across, step)

            def wait_near(row):
                for t in range(per_dev):
                    when(held(row, partner, t), lambda t=t: share(row, t, partner).wait_recv())

            def half_product(side, start, stop):
                total = None
                for t in range(per_dev):
                    depth = pl.ds(pl.multiple_of((side + group * t) * BLOCK, 2 * BLOCK), 2 * BLOCK)
                    term = jnp.dot(l_refs[last][:, depth], b_vmem[depth, start:stop], preferred_element_type=jnp.float32)
                    total = term if total is None else total + term
                return total

            def multiply(row, start, stop):
                if row == last:
                    for n in range(start, stop, TILE):
                        total = partial[:, n:n + TILE] + half_product(far, n, n + TILE)
                        x_refs[row][:, n:n + TILE] = total.astype(dtype)
                    return
                x_refs[row][:, start:stop] = jnp.dot(
                    l_refs[row][...], b_vmem[:(row + 1) * BLOCK, start:stop],
                    preferred_element_type=jnp.float32).astype(dtype)

            wait_near(last)
            wait_side(0)
            middle = EARLY // (2 * TILE) * TILE
            for start in range(0, EARLY, TILE):
                if start == middle:
                    relay(sequence[0])
                partial[:, start:start + TILE] = half_product(near, start, start + TILE)
            wait_side(1)

            freed = []
            for place, row in enumerate(sequence):
                if row != last:
                    wait_near(row)
                for t in range(per_dev):
                    parts(row, t, diagonal, f_send, f_recv, partner, lambda j, copy: copy.wait_recv())
                split = before[place] * TILE
                if split:
                    multiply(row, 0, split)
                if place + 1 < n_rows:
                    relay(sequence[place + 1])
                multiply(row, split, EARLY)
                free = [k for k in range(n_rows // 2, n_rows) if all(k > r for r in sequence[place + 1:])]
                for k in free:
                    if k not in freed:
                        freed.append(k)
                        for piece in range(2 * (last - k), 2 * (n_rows - k)):
                            load_late(piece).start()

            like = b_vmem.at[:, pl.ds(0, late)]
            pltpu.make_async_copy(like, like, late_sem).wait()
            wait_all(x_send, me, True)
            wait_all(p_send, me, False)
            wait_all(f_send, across, True)

        dma = pltpu.SemaphoreType.DMA
        vmem = pl.BlockSpec(memory_space=pltpu.VMEM)
        hbm = pl.BlockSpec(memory_space=pltpu.HBM)
        gathered = pl.pallas_call(
            gather_kernel,
            out_shape=tuple(pltpu.VMEM((BLOCK, EARLY), dtype) for _ in range(n_rows))
            + tuple(pltpu.VMEM((BLOCK, BLOCK * (i + 1)), dtype) for i in range(n_rows))
            + (pltpu.VMEM((order, EARLY), dtype),),
            in_specs=[hbm, hbm],
            out_specs=(vmem,) * (2 * n_rows + 1),
            scratch_shapes=[pltpu.VMEM((BLOCK, EARLY), jnp.float32), dma((2,)), dma, dma,
                            dma, dma((2 * n_rows - group,)), dma, dma((3 * n_rows - group,)), dma, dma((3 * n_rows - group,))],
            compiler_params=pltpu.CompilerParams(
                collective_id=0, has_side_effects=True, vmem_limit_bytes=8 * MIB),
            name="gather_and_multiply",
        )(l_cols, b_cols)

        def finish_kernel(*refs):
            x_refs, l_refs = refs[:n_rows], refs[n_rows:2 * n_rows]
            b_vmem, out_ref, x_vmem, x_sem, early_sem = refs[2 * n_rows:]

            def put_early(row):
                return pltpu.make_async_copy(
                    x_refs[row], out_ref.at[pl.ds(row * BLOCK, BLOCK), pl.ds(0, EARLY)], early_sem)

            def put_late(n, row):
                rows = pl.ds(row * BLOCK, BLOCK)
                cols = pl.ds(EARLY + n * TILE, TILE)
                slot = n % 2
                return pltpu.make_async_copy(x_vmem.at[slot, rows, :], out_ref.at[rows, cols], x_sem.at[slot])

            def wait_tile(n):
                like = x_vmem.at[n % 2]
                pltpu.make_async_copy(like, like, x_sem.at[n % 2]).wait()

            for row in range(n_rows - 1, 4, -1):
                put_early(row).start()

            for n in range(n_late):
                for row in range(5):
                    if n == 1 + row // 2:
                        put_early(row).start()
                if n >= 2:
                    wait_tile(n - 2)
                for row in range(n_rows - 1, -1, -1):
                    total = None
                    for k in range(row + 1):
                        rows, start = late_place(k)
                        term = jnp.dot(l_refs[row][:, k * BLOCK:(k + 1) * BLOCK],
                                       b_vmem[rows, start + n * TILE:start + (n + 1) * TILE],
                                       preferred_element_type=jnp.float32)
                        total = term if total is None else total + term
                    x_vmem[n % 2, row * BLOCK:(row + 1) * BLOCK, :] = total.astype(dtype)
                    put_late(n, row).start()

            like = b_vmem
            pltpu.make_async_copy(like, like, early_sem).wait()
            for n in range(n_late - 2, n_late):
                wait_tile(n)

        return pl.pallas_call(
            finish_kernel,
            out_shape=jax.ShapeDtypeStruct((order, width), dtype),
            in_specs=[vmem] * (2 * n_rows + 1),
            out_specs=hbm,
            scratch_shapes=[pltpu.VMEM((2, order, TILE), dtype), dma((2,)), dma],
            compiler_params=pltpu.CompilerParams(vmem_limit_bytes=5 * MIB),
            name="finish",
        )(*gathered)

    return jax.shard_map(local_product, mesh=mesh, in_specs=(P("batch", "col"), P("batch", "col")), out_specs=P("batch", "col"), check_vma=False)
```

```python
import jax
import jax.numpy as jnp
from jax import lax
from jax.experimental import pallas as pl
from jax.experimental.pallas import tpu as pltpu
from jax.sharding import PartitionSpec as P

BLOCK = 256
MESH = pl.DeviceIdType.MESH
MIB = 1024 * 1024
EARLY = 5632
TILE = 512


def when(cond, fn):
    if cond is True:
        fn()
    elif cond is not False:
        pl.when(cond)(fn)


def solution(mesh):
    group = mesh.shape["col"]

    def local_product(l_cols, b_cols):
        order, local_width = l_cols.shape
        width = b_cols.shape[1]
        per_dev = local_width // BLOCK
        n_rows = order // BLOCK
        late = width - EARLY
        n_late = late // TILE
        dtype = b_cols.dtype

        def held(row, owner, t):
            low, high = group * t, group * t + group - 1
            if row >= high:
                return True
            if row < low:
                return False
            return owner + low <= row

        def pieces(row, t, owner):
            full = [(0, BLOCK, BLOCK)]
            high = row - group * t
            if high >= group:
                return [(True, full)]
            if high < 0:
                return []
            half = BLOCK // 2
            cases = [(owner == high, [(0, half, half), (half, half, BLOCK)])]
            if high > 0:
                cases.append((owner < high, full))
            return cases

        def late_place(k):
            return pl.ds((n_rows - 1 - k // 2) * BLOCK, BLOCK), (k % 2) * late

        def gather_kernel(l_ref, b_ref, *refs):
            x_refs, l_refs = refs[:n_rows], refs[n_rows:2 * n_rows]
            b_vmem, partial, b_sem, late_sem, own_sem, p_send, p_recv, x_send, x_recv, f_send, f_recv = refs[2 * n_rows:]
            me = lax.axis_index("col")
            across = lax.rem(me + 2, group)
            partner = me + 1 - 2 * lax.rem(me, 2)
            diagonal = lax.rem(partner + 2, group)

            def panel(row, owner, t):
                start = pl.multiple_of((owner + group * t) * BLOCK, BLOCK)
                return l_refs[row].at[:, pl.ds(start, BLOCK)]

            def mine(row, t):
                return l_ref.at[pl.ds(row * BLOCK, BLOCK), pl.ds(t * BLOCK, BLOCK)]

            def own_copy(row, t):
                return pltpu.make_async_copy(mine(row, t), panel(row, me, t), own_sem)

            def wait_all(sem, owner, halves):
                for c in range(group):
                    width = (2 * n_rows - group - 2 * c) * BLOCK - (BLOCK // 2 if halves else 0)
                    like = x_refs[last].at[:, pl.ds(0, width)]
                    pl.when(owner == c)(lambda like=like: pltpu.make_async_copy(like, like, sem).wait())

            def wait_row(sem, row, owner):
                for c in range(group):
                    size = sum(rows * width for t in range(per_dev) for cond, rects in pieces(row, t, c) if cond
                               for _, rows, width in rects)
                    if size:
                        like = b_vmem.at[pl.ds(0, size // BLOCK), pl.ds(0, BLOCK)]
                        pl.when(owner == c)(lambda like=like: pltpu.make_async_copy(like, like, sem.at[row]).wait())

            last = n_rows - 1

            def remote(src, dst, send_sem, recv_sem, peer):
                return pltpu.make_async_remote_copy(
                    src_ref=src, dst_ref=dst, send_sem=send_sem, recv_sem=recv_sem, device_id={"col": peer}, device_id_type=MESH)

            def share(row, t, owner):
                block = panel(row, owner, t)
                return remote(block, block, p_send, p_recv.at[0 if row == last else 1], partner)

            def parts(row, t, owner, send_sem, recv_sem, peer, act):
                for cond, rects in pieces(row, t, owner):
                    def run(rects=rects):
                        for j, (first, rows, width) in enumerate(rects):
                            start = pl.multiple_of((owner + group * t) * BLOCK, BLOCK)
                            part = l_refs[row].at[pl.ds(first, rows), pl.ds(start, width)]
                            act(j, remote(part, part, send_sem, recv_sem.at[row], peer))
                    when(cond, run)

            def parts_both(row, t, owner, act):
                for cond, rects in pieces(row, t, owner):
                    def run(rects=rects):
                        for j, (first, rows, width) in enumerate(rects):
                            start = pl.multiple_of((owner + group * t) * BLOCK, BLOCK)
                            part = l_refs[row].at[pl.ds(first, rows), pl.ds(start, width)]
                            act(remote(part, part, f_send, f_recv.at[row], partner))
                    when(cond, run)

            near = me - lax.rem(me, 2)
            far = 2 - near

            def load_b(k, sem):
                rows = pl.ds(pl.multiple_of(k * BLOCK, BLOCK), BLOCK)
                return pltpu.make_async_copy(b_ref.at[rows, pl.ds(0, EARLY)], b_vmem.at[rows, :], sem)

            def wait_side(i):
                like = b_vmem.at[pl.ds(0, n_rows // 2 * BLOCK), :]
                pltpu.make_async_copy(like, like, b_sem.at[i]).wait()

            def load_late(k):
                rows, start = late_place(k)
                return pltpu.make_async_copy(
                    b_ref.at[pl.ds(k * BLOCK, BLOCK), pl.ds(EARLY, late)], b_vmem.at[rows, pl.ds(start, late)], late_sem)

            sequence = [3, 6, 5, 4, 7, 2, 1, 0]
            before = [8, 8, 8, 8, 5, 5, 0, 0]
            blocks = [(row, t) for row in sequence for t in range(per_dev)]
            shared = [(last, t) for t in range(per_dev)] + [b for b in blocks if b[0] != last]

            barrier = pltpu.get_barrier_semaphore()
            for peer in (partner, across):
                pl.semaphore_signal(barrier, inc=1, device_id={"col": peer}, device_id_type=MESH)
            for row, t in shared:
                when(held(row, me, t), lambda row=row, t=t: own_copy(row, t).start())
            for row in range(n_rows):
                def clear(row=row):
                    l_refs[row][:BLOCK // 2, row * BLOCK + BLOCK // 2:] = jnp.zeros((BLOCK // 2, BLOCK // 2), dtype)
                when(far == row % group // 2 * 2, clear)
            wait_all(own_sem, me, False)
            for i, side in enumerate((near, far)):
                for t in range(per_dev):
                    for c in range(2):
                        load_b(side + group * t + c, b_sem.at[i]).start()
            pl.semaphore_wait(barrier, 2)

            for row, t in blocks:
                parts(row, t, me, x_send, x_recv, across, lambda j, copy: copy.start())
            for row, t in shared:
                when(held(row, me, t), lambda row=row, t=t: share(row, t, me).start())

            def relay(row):
                wait_row(x_recv, row, across)
                for t in range(per_dev):
                    parts_both(row, t, across, lambda copy: copy.start())

            def wait_near(rest):
                for c in range(group):
                    width = (2 * n_rows - group - 2 * c - per_dev if rest else per_dev) * BLOCK
                    like = x_refs[last].at[:, pl.ds(0, width)]
                    pl.when(partner == c)(lambda like=like: pltpu.make_async_copy(like, like, p_recv.at[rest]).wait())

            def half_product(side, start, stop):
                total = None
                for t in range(per_dev):
                    depth = pl.ds(pl.multiple_of((side + group * t) * BLOCK, 2 * BLOCK), 2 * BLOCK)
                    term = jnp.dot(l_refs[last][:, depth], b_vmem[depth, start:stop], preferred_element_type=jnp.float32)
                    total = term if total is None else total + term
                return total

            def multiply(row, start, stop):
                if row == last:
                    for n in range(start, stop, TILE):
                        total = partial[:, n:n + TILE] + half_product(far, n, n + TILE)
                        x_refs[row][:, n:n + TILE] = total.astype(dtype)
                    return
                x_refs[row][:, start:stop] = jnp.dot(
                    l_refs[row][...], b_vmem[:(row + 1) * BLOCK, start:stop],
                    preferred_element_type=jnp.float32).astype(dtype)

            wait_near(0)
            wait_side(0)
            middle = EARLY // (2 * TILE) * TILE
            for start in range(0, EARLY, TILE):
                if start == middle:
                    relay(sequence[0])
                partial[:, start:start + TILE] = half_product(near, start, start + TILE)
            wait_side(1)

            freed = []
            for place, row in enumerate(sequence):
                if place == 0:
                    wait_near(1)
                wait_row(f_recv, row, diagonal)
                split = before[place] * TILE
                if split:
                    multiply(row, 0, split)
                if place + 1 < n_rows:
                    relay(sequence[place + 1])
                multiply(row, split, EARLY)
                free = [k for k in range(n_rows // 2, n_rows) if all(k > r for r in sequence[place + 1:])]
                for k in free:
                    if k not in freed:
                        freed.append(k)
                        for piece in range(2 * (last - k), 2 * (n_rows - k)):
                            load_late(piece).start()

            like = b_vmem.at[:, pl.ds(0, late)]
            pltpu.make_async_copy(like, like, late_sem).wait()
            wait_all(x_send, me, True)
            wait_all(p_send, me, False)
            wait_all(f_send, across, True)

        dma = pltpu.SemaphoreType.DMA
        vmem = pl.BlockSpec(memory_space=pltpu.VMEM)
        hbm = pl.BlockSpec(memory_space=pltpu.HBM)
        gathered = pl.pallas_call(
            gather_kernel,
            out_shape=tuple(pltpu.VMEM((BLOCK, EARLY), dtype) for _ in range(n_rows))
            + tuple(pltpu.VMEM((BLOCK, BLOCK * (i + 1)), dtype) for i in range(n_rows))
            + (pltpu.VMEM((order, EARLY), dtype),),
            in_specs=[hbm, hbm],
            out_specs=(vmem,) * (2 * n_rows + 1),
            scratch_shapes=[pltpu.VMEM((BLOCK, EARLY), jnp.float32), dma((2,)), dma, dma,
                            dma, dma((2,)), dma, dma((n_rows,)), dma, dma((n_rows,))],
            compiler_params=pltpu.CompilerParams(
                collective_id=0, has_side_effects=True, vmem_limit_bytes=8 * MIB),
            name="gather_and_multiply",
        )(l_cols, b_cols)

        def finish_kernel(*refs):
            x_refs, l_refs = refs[:n_rows], refs[n_rows:2 * n_rows]
            b_vmem, out_ref, x_vmem, x_sem, early_sem = refs[2 * n_rows:]

            def put_early(row):
                return pltpu.make_async_copy(
                    x_refs[row], out_ref.at[pl.ds(row * BLOCK, BLOCK), pl.ds(0, EARLY)], early_sem)

            def put_late(n, row):
                rows = pl.ds(row * BLOCK, BLOCK)
                cols = pl.ds(EARLY + n * TILE, TILE)
                slot = n % 2
                return pltpu.make_async_copy(x_vmem.at[slot, rows, :], out_ref.at[rows, cols], x_sem.at[slot])

            def wait_tile(n):
                like = x_vmem.at[n % 2]
                pltpu.make_async_copy(like, like, x_sem.at[n % 2]).wait()

            for row in range(n_rows - 1, 4, -1):
                put_early(row).start()

            for n in range(n_late):
                for row in range(5):
                    if n == 1 + row // 2:
                        put_early(row).start()
                if n >= 2:
                    wait_tile(n - 2)
                for row in range(n_rows - 1, -1, -1):
                    total = None
                    for k in range(row + 1):
                        rows, start = late_place(k)
                        term = jnp.dot(l_refs[row][:, k * BLOCK:(k + 1) * BLOCK],
                                       b_vmem[rows, start + n * TILE:start + (n + 1) * TILE],
                                       preferred_element_type=jnp.float32)
                        total = term if total is None else total + term
                    x_vmem[n % 2, row * BLOCK:(row + 1) * BLOCK, :] = total.astype(dtype)
                    put_late(n, row).start()

            like = b_vmem
            pltpu.make_async_copy(like, like, early_sem).wait()
            for n in range(n_late - 2, n_late):
                wait_tile(n)

        return pl.pallas_call(
            finish_kernel,
            out_shape=jax.ShapeDtypeStruct((order, width), dtype),
            in_specs=[vmem] * (2 * n_rows + 1),
            out_specs=hbm,
            scratch_shapes=[pltpu.VMEM((2, order, TILE), dtype), dma((2,)), dma],
            compiler_params=pltpu.CompilerParams(vmem_limit_bytes=5 * MIB),
            name="finish",
        )(*gathered)

    return jax.shard_map(local_product, mesh=mesh, in_specs=(P("batch", "col"), P("batch", "col")), out_specs=P("batch", "col"), check_vma=False)
```
